128 devices in a mesh: gx: 8 (over z, y_hi), gy: 16 (over x, y_lo, core).
Axes of the slice: x: 4, y: 4 (y_hi: 2, y_lo: 2; y = y_hi * 2 + y_lo), z: 4, core: 2. Of those that a mesh axis runs over, the one named last changes fastest.
Arguments:
- node_coords: float32 [49152, 3, 128], P(('gx', 'gy')), may hold values from -6 to 6
- node_disp: float32 [49152, 3, 128], P(('gx', 'gy')), may hold values from -6 to 6
- qpoints: float32 [32768, 3, 256], P(('gx', 'gy')), may hold values from -6 to 6
- qweights: float32 [32768, 256], P(('gx', 'gy')), may hold values from 0.1 to 2
- qcount: int32 [32768], P(('gx', 'gy')), may hold values from 64 to 256
- sec_block: int32 [32768], P(('gx', 'gy')), may hold values from 0 to 49151, as said below
- pri_block: int32 [32768], P(('gx', 'gy')), may hold values from 0 to 49151, as said below
Outputs:
- gap: float32 [49152, 3, 128], P(('gx', 'gy'))
The draws below stay inside these ranges and needn't reach their ends.
Inputs may be any that keep to these rules, and one draw needn't show every extreme that they name: `sec_block`: patch b is owned by device b // 384. Among the segments of one device, at most 4 have their secondary patch owned by any one device; in every draw some device owns the secondary patches of exactly 4 segments of every device. `pri_block`: as for sec_block, with primary patches: at most 4 segments of one device name patches of any one owner, and some owner gets exactly 4 from every device.
All inputs are finite; a program needn't handle non-finite values.
Results may differ from the reference program's by a relative error of at most 0.000098.
Values sent between devices are 32-bit elements; how exact they have to be, the bound alone decides.
No kernel may reach another device: no remote copies, remote signals or barrier semaphores. Data moves between devices by JAX's collectives and lax.ppermute only.
A program may use at most 64 MiB of HBM per device.

```python
import math
import jax
import jax.numpy as jnp
from jax import lax

NPB = 128
Q = 256
SEG_DEV = 256
NB_DEV = 384
NDEV = 128
CAP = 4
SEGMENTS = 32768
NB = 49152


def owner_routes(key):
    slot_count = NDEV * CAP
    hot_owner = jax.random.randint(jax.random.fold_in(key, 5), (), 0, NDEV)
    device_keys = jax.random.split(jax.random.fold_in(key, 7), NDEV)

    def one_device(dev_key):
        first, second, third = jax.random.split(dev_key, 3)
        positions = jnp.arange(slot_count, dtype=jnp.int32)
        scores = jax.random.randint(first, (slot_count,), 0, 65536) * slot_count + positions
        scores = jnp.where(positions // CAP == hot_owner, scores + 2 ** 30, scores)
        chosen = jax.lax.top_k(scores, SEG_DEV)[1]
        owners = (chosen // CAP).astype(jnp.int32)
        owners = jax.random.permutation(second, owners)
        local_ids = jax.random.randint(third, (SEG_DEV,), 0, NB_DEV)
        return owners * NB_DEV + local_ids
    return jax.vmap(one_device)(device_keys).reshape(-1).astype(jnp.int32)


def draw_sec_block(key, part):
    return owner_routes(jax.random.fold_in(key, 11))


def draw_pri_block(key, part):
    return owner_routes(jax.random.fold_in(key, 23))


def set_ends(array, key, least, high):
    longest = array.shape.index(max(array.shape))
    spots = []
    for shift in (0, 1):
        where = [jax.random.randint(jax.random.fold_in(key, axis), (), 0, length) for axis, length in enumerate(array.shape)]
        where[longest] = (where[longest] + shift) % array.shape[longest]
        spots.append(tuple(where))
    return array.at[spots[0]].set(least).at[spots[1]].set(high)


def levels(stream_key, dims, cuts, smallest, largest):
    gain = 1.0
    for dim, blocks in cuts:
        steps = jax.random.uniform(jax.random.fold_in(jax.random.fold_in(stream_key, 6), dim), (blocks,), jnp.float32, smallest / len(cuts), largest / len(cuts))
        gain = gain * jnp.repeat(jnp.exp(steps), dims[dim] // blocks).reshape((-1,) + (1,) * (len(dims) - 1 - dim))
    return gain


def normal_values(key, shape, width, limit, pieces=(), kind=jnp.bfloat16):
    values = jax.random.normal(key, shape, jnp.float32) * width
    if len(pieces) > 0:
        values = levels(key, shape, pieces, -0.22, 0.18) * values
    return jnp.clip(values, min=-limit, max=limit).astype(kind)


def setup_inputs(seed: int = 0) -> dict:
    keys = jax.random.split(jax.random.key(seed), 8)
    node_coords = normal_values(keys[0], (NB, 3, NPB), 1.0, 6.0, ((0, 128),), jnp.float32)
    node_disp = normal_values(keys[1], (NB, 3, NPB), 1.0, 6.0, ((0, 128),), jnp.float32)
    qpoints = normal_values(keys[2], (SEGMENTS, 3, Q), 1.0, 6.0, ((0, 128),), jnp.float32)
    qweights = jnp.clip(jnp.exp(math.log(2.0) - 2.9957323 * jax.random.uniform(keys[3], (SEGMENTS, Q), jnp.float32) ** levels(keys[3], (SEGMENTS, Q), ((0, 128),), -0.2, 0.2)), 0.1, 2.0)
    qcount = set_ends(jax.random.randint(keys[4], (SEGMENTS,), Q // 4, Q + 1), jax.random.fold_in(keys[4], 1), Q // 4, Q).astype(jnp.int32)
    sec_block = draw_sec_block(jax.random.fold_in(keys[7], 71), 0)
    pri_block = draw_pri_block(jax.random.fold_in(keys[7], 71), 0)
    return {"node_coords": node_coords, "node_disp": node_disp, "qpoints": qpoints, "qweights": qweights, "qcount": qcount, "sec_block": sec_block, "pri_block": pri_block}


def shape_values(points, coords):
    diff0 = points[:, 0, :, None] - coords[:, 0, None, :]
    diff1 = points[:, 1, :, None] - coords[:, 1, None, :]
    diff2 = points[:, 2, :, None] - coords[:, 2, None, :]
    radius = diff0 * diff0 + diff1 * diff1 + diff2 * diff2
    kernel = 1.0 / (1.0 + 2.0 * radius)
    return kernel / jnp.sum(kernel, axis=-1, keepdims=True)


def reference(node_coords, node_disp, qpoints, qweights, qcount, sec_block, pri_block):
    node_data = jnp.concatenate([node_coords, node_disp], axis=1)
    live = jnp.arange(Q, dtype=jnp.int32)[None, :] < qcount[:, None]
    weights = jnp.where(live, qweights, jnp.zeros_like(qweights))
    seg_group = 64
    groups = SEGMENTS // seg_group
    hp = lax.Precision.HIGHEST

    def one_group(inputs):
        points, quad_weights, sec_ids, pri_ids = inputs
        sec_nodes = jnp.take(node_data, sec_ids, axis=0)
        pri_nodes = jnp.take(node_data, pri_ids, axis=0)
        sec_shape = shape_values(points, sec_nodes[:, :3])
        pri_shape = shape_values(points, pri_nodes[:, :3])
        weighted = quad_weights[:, :, None] * sec_shape
        mismatch = jnp.einsum("gqj,gcj->gcq", sec_shape, sec_nodes[:, 3:], precision=hp) - jnp.einsum("gqj,gcj->gcq", pri_shape, pri_nodes[:, 3:], precision=hp)
        return jnp.einsum("gqk,gcq->gck", weighted, mismatch, precision=hp)

    contrib = lax.map(one_group, (qpoints.reshape(groups, seg_group, 3, Q), weights.reshape(groups, seg_group, Q), sec_block.reshape(groups, seg_group), pri_block.reshape(groups, seg_group)))
    contrib = contrib.reshape(SEGMENTS, 3, NPB)
    return jax.ops.segment_sum(contrib, sec_block, num_segments=NB)
```

```python
import functools
import jax
import jax.numpy as jnp
from jax import lax
from jax.experimental import pallas as pl
from jax.experimental.pallas import tpu as pltpu
from jax.sharding import PartitionSpec as P

AXES = ("gx", "gy")
GROUP = 8


def routing(block_ids, blocks_dev, capacity, slot_count):
    owners = block_ids // blocks_dev
    local_ids = block_ids % blocks_dev
    positions = jnp.arange(block_ids.shape[0], dtype=jnp.int32)
    same_owner = (owners[:, None] == owners[None, :]) & (positions[:, None] > positions[None, :])
    ranks = jnp.sum(same_owner.astype(jnp.int32), axis=1)
    slot_ids = owners * capacity + ranks
    matches = slot_ids[:, None] == jnp.arange(slot_count, dtype=jnp.int32)[None, :]
    request = jnp.sum(jnp.where(matches, local_ids[:, None], 0), axis=0)
    return (slot_ids, request)


def gather_kernel(devices, capacity, blocks, ids_ref, xc_ref, xu_ref, sec_ref, pri_ref):
    rows = 6 * capacity

    def one_device(dev, carry):
        for side, out in ((0, sec_ref), (1, pri_ref)):
            for rank in range(capacity):
                local = ids_ref[side * devices * capacity + dev * capacity + rank]
                base = dev * rows + rank
                out[pl.ds(base, 3, stride=capacity), :] = xc_ref[pl.ds(local, 3, stride=blocks), :]
                out[pl.ds(base + 3 * capacity, 3, stride=capacity), :] = xu_ref[
                    pl.ds(local, 3, stride=blocks), :
                ]
        return carry

    lax.fori_loop(0, devices, one_device, 0)


def pieces(value):
    first = value.astype(jnp.bfloat16).astype(jnp.float32)
    rest = value - first
    second = rest.astype(jnp.bfloat16).astype(jnp.float32)
    return (first, second, rest - second)


def node_side(fetched_ref, slot, capacity):
    dev = slot // capacity
    rank = slot % capacity
    raw = fetched_ref[pl.ds(dev * (6 * capacity) + rank, 6, stride=capacity), :]
    raw = jnp.concatenate([raw, jnp.zeros((2, raw.shape[1]), jnp.float32)], axis=0)
    row = lax.broadcasted_iota(jnp.int32, raw.shape, 0)
    coord = jnp.where(row < 3, raw, 0.0)
    square = 2.0 * jnp.sum(coord * coord, axis=0, keepdims=True)
    extended = jnp.where(row == 3, square, jnp.where(row == 4, 1.0, -4.0 * coord))
    a, b, c = pieces(extended)
    stacked = jnp.concatenate([a, a, b, b, a, c], axis=0)
    disp = jnp.where(row < 3, 0.0, jnp.where(row == 6, 1.0, raw))
    high = disp.astype(jnp.bfloat16).astype(jnp.float32)
    lhs = jnp.concatenate([high, disp - high], axis=0)
    lhs = jnp.concatenate([lhs, lhs], axis=1).astype(jnp.bfloat16)
    return stacked.T.astype(jnp.bfloat16), lhs


def point_side(points):
    a, b, c = pieces(points)
    return jnp.concatenate([a, b, a, b, c, a], axis=0).astype(jnp.bfloat16)


def kernel_values(node_op, point_op):
    dist = jnp.dot(node_op, point_op, preferred_element_type=jnp.float32)
    value = 1.0 / dist
    high = value.astype(jnp.bfloat16)
    low = (value - high.astype(jnp.float32)).astype(jnp.bfloat16)
    return jnp.concatenate([high, low], axis=0)


def pri_kernel(capacity, slots_ref, fetched_ref, points_ref, out_ref):
    def one_group(g, carry):
        for i in range(GROUP):
            s = g * GROUP + i
            node_op, lhs = node_side(fetched_ref, slots_ref[s], capacity)
            both = kernel_values(node_op, point_side(points_ref[s]))
            sums = jnp.dot(lhs, both, preferred_element_type=jnp.float32)
            sums = sums[:8] + sums[8:]
            out_ref[s] = sums * (1.0 / sums[6:7])
        return carry

    lax.fori_loop(0, points_ref.shape[0] // GROUP, one_group, 0)


def sec_kernel(capacity, slots_ref, fetched_ref, points_ref, other_ref, out_ref):
    out_ref[...] = jnp.zeros_like(out_ref)

    def one_group(g, carry):
        for i in range(GROUP):
            s = g * GROUP + i
            slot = slots_ref[s]
            points = points_ref[s]
            node_op, lhs = node_side(fetched_ref, slot, capacity)
            both = kernel_values(node_op, point_side(points))
            sums = jnp.dot(lhs, both, preferred_element_type=jnp.float32)
            sums = sums[:8] + sums[8:]
            inverse = 1.0 / sums[6:7]
            gap = (points[5:6] * inverse) * (sums * inverse - other_ref[s])
            high = gap.astype(jnp.bfloat16).astype(jnp.float32)
            left = jnp.concatenate([high, gap - high], axis=0).astype(jnp.bfloat16)
            result = lax.dot_general(
                left, both, (((1,), (1,)), ((), ())), preferred_element_type=jnp.float32
            )
            half = result.shape[1] // 2
            result = result[:8] + result[8:]
            result = result[:, :half] + result[:, half:]
            dev = slot // capacity
            base = dev * (3 * capacity) + slot % capacity
            out_ref[pl.ds(base, 3, stride=capacity), :] = result[3:6]
        return carry

    lax.fori_loop(0, points_ref.shape[0] // GROUP, one_group, 0)


def body(node_coords, node_disp, qpoints, qweights, qcount, sec_block, pri_block):
    devices = lax.axis_size("gx") * lax.axis_size("gy")
    blocks = node_coords.shape[0]
    nodes = node_coords.shape[2]
    segs = qpoints.shape[0]
    quad = qpoints.shape[2]
    slots = 2 * segs
    cap = slots // devices
    f32 = jnp.float32
    smem = pl.BlockSpec(memory_space=pltpu.SMEM)
    vmem = pl.BlockSpec(memory_space=pltpu.VMEM)

    def exchange(value):
        return lax.all_to_all(value, AXES, split_axis=0, concat_axis=0, tiled=True)

    sec_slots, sec_request = routing(sec_block, blocks, cap, slots)
    pri_slots, pri_request = routing(pri_block, blocks, cap, slots)
    requests = jnp.concatenate(
        [sec_request.reshape(devices, cap), pri_request.reshape(devices, cap)], axis=1
    )
    received = exchange(requests)
    sec_ids = received[:, :cap].reshape(slots)
    ids = jnp.concatenate([sec_ids, received[:, cap:].reshape(slots)])

    xc = jnp.transpose(node_coords, (1, 0, 2)).reshape(3 * blocks, nodes)
    xu = jnp.transpose(node_disp, (1, 0, 2)).reshape(3 * blocks, nodes)
    sendable = jax.ShapeDtypeStruct((devices * 6 * cap, nodes), f32)
    sec_out, pri_out = pl.pallas_call(
        functools.partial(gather_kernel, devices, cap, blocks),
        out_shape=(sendable, sendable),
        in_specs=[smem, vmem, vmem],
        out_specs=(vmem, vmem),
    )(ids, xc, xu)
    pri_in = exchange(pri_out.reshape(devices, 6 * cap, nodes)).reshape(-1, nodes)
    sec_in = exchange(sec_out.reshape(devices, 6 * cap, nodes)).reshape(-1, nodes)

    live = jnp.arange(quad, dtype=jnp.int32)[None, :] < qcount[:, None]
    weights = jnp.where(live, qweights, jnp.zeros_like(qweights))
    qx, qy, qz = qpoints[:, 0], qpoints[:, 1], qpoints[:, 2]
    ones = jnp.ones_like(qx)
    zeros = jnp.zeros_like(qx)
    square = 1.0 + 2.0 * (qx * qx + qy * qy + qz * qz)
    points = jnp.stack([qx, qy, qz, ones, square, weights, zeros, zeros], axis=1)

    other = pl.pallas_call(
        functools.partial(pri_kernel, cap),
        out_shape=jax.ShapeDtypeStruct((segs, 8, quad), f32),
        in_specs=[smem, vmem, vmem],
        out_specs=vmem,
    )(pri_slots, pri_in, points)
    parcels = pl.pallas_call(
        functools.partial(sec_kernel, cap),
        out_shape=jax.ShapeDtypeStruct((devices * 3 * cap, nodes), f32),
        in_specs=[smem, vmem, vmem, vmem],
        out_specs=vmem,
    )(sec_slots, sec_in, points, other)
    incoming = exchange(parcels.reshape(devices, 3 * cap, nodes))
    incoming = incoming.reshape(devices, 3, cap, nodes)
    select = (jnp.arange(blocks, dtype=jnp.int32)[:, None] == sec_ids[None, :]).astype(f32)
    incoming = jnp.transpose(incoming, (0, 2, 1, 3)).reshape(slots, 3, nodes)
    return jnp.einsum("bp,pcn->bcn", select, incoming, precision=lax.Precision.HIGHEST)


def solution(mesh):
    split3 = P(AXES, None, None)
    placed = (split3, split3, split3, P(AXES, None), P(AXES), P(AXES), P(AXES))
    return jax.shard_map(body, mesh=mesh, in_specs=placed, out_specs=split3, check_vma=False)
```

```python
import functools
import jax
import jax.numpy as jnp
from jax import lax
from jax.experimental import pallas as pl
from jax.experimental.pallas import tpu as pltpu
from jax.sharding import PartitionSpec as P

AXES = ("gx", "gy")
HALF = 8


def routing(block_ids, blocks_dev, capacity, slot_count):
    owners = block_ids // blocks_dev
    local_ids = block_ids % blocks_dev
    positions = jnp.arange(block_ids.shape[0], dtype=jnp.int32)
    same_owner = (owners[:, None] == owners[None, :]) & (positions[:, None] > positions[None, :])
    ranks = jnp.sum(same_owner.astype(jnp.int32), axis=1)
    slot_ids = owners * capacity + ranks
    matches = slot_ids[:, None] == jnp.arange(slot_count, dtype=jnp.int32)[None, :]
    request = jnp.sum(jnp.where(matches, local_ids[:, None], 0), axis=0)
    return (slot_ids, request)


def gather_kernel(devices, capacity, blocks, ids_ref, xc_ref, xu_ref, out_ref):
    rows = 6 * capacity

    def one_device(dev, carry):
        for rank in range(capacity):
            local = ids_ref[dev * capacity + rank]
            base = dev * rows + rank
            out_ref[pl.ds(base, 3, stride=capacity), :] = xc_ref[pl.ds(local, 3, stride=blocks), :]
            out_ref[pl.ds(base + 3 * capacity, 3, stride=capacity), :] = xu_ref[
                pl.ds(local, 3, stride=blocks), :
            ]
        return carry

    lax.fori_loop(0, devices, one_device, 0, unroll=4)


def pieces(value):
    first = value.astype(jnp.bfloat16).astype(jnp.float32)
    rest = value - first
    second = rest.astype(jnp.bfloat16).astype(jnp.float32)
    return (first, second, rest - second)


def node_side(fetched_ref, slot, capacity):
    dev = slot // capacity
    rank = slot % capacity
    raw = fetched_ref[pl.ds(dev * (6 * capacity) + rank, 6, stride=capacity), :]
    raw = jnp.concatenate([raw, jnp.zeros((2, raw.shape[1]), jnp.float32)], axis=0)
    row = lax.broadcasted_iota(jnp.int32, raw.shape, 0)
    coord = jnp.where(row < 3, raw, 0.0)
    square = 2.0 * jnp.sum(coord * coord, axis=0, keepdims=True)
    extended = jnp.where(row == 3, square, jnp.where(row == 4, 1.0, -4.0 * coord))
    a, b, c = pieces(extended)
    stacked = jnp.concatenate([a, a, b, b, a, c], axis=0)
    disp = jnp.where(row < 3, 0.0, jnp.where(row == 6, 1.0, raw))
    high = disp.astype(jnp.bfloat16).astype(jnp.float32)
    lhs = jnp.concatenate([high, disp - high], axis=0)
    lhs = jnp.concatenate([lhs, lhs], axis=1).astype(jnp.bfloat16)
    return stacked.T.astype(jnp.bfloat16), lhs


def point_side(points):
    a, b, c = pieces(points)
    return jnp.concatenate([a, b, a, b, c, a], axis=0).astype(jnp.bfloat16)


def kernel_values(node_op, point_op):
    dist = jnp.dot(node_op, point_op, preferred_element_type=jnp.float32)
    value = 1.0 / dist
    high = value.astype(jnp.bfloat16)
    low = (value - high.astype(jnp.float32)).astype(jnp.bfloat16)
    return jnp.concatenate([high, low], axis=0)


def stage_a(capacity, s, slot, fetched_ref, points_ref, both_ref, lhs_ref, i):
    node_op, lhs = node_side(fetched_ref, slot, capacity)
    lhs_ref[i] = lhs
    both_ref[i] = kernel_values(node_op, point_side(points_ref[s]))


def sums_of(both_ref, lhs_ref, i):
    sums = jnp.dot(lhs_ref[i], both_ref[i], preferred_element_type=jnp.float32)
    return sums[:8] + sums[8:]


def pri_kernel(capacity, slots_ref, fetched_ref, points_ref, out_ref, both_ref, lhs_ref):
    segs = points_ref.shape[0]

    def first(s, i):
        stage_a(capacity, s, slots_ref[s], fetched_ref, points_ref, both_ref, lhs_ref, i)

    def second(s, i):
        sums = sums_of(both_ref, lhs_ref, i)
        out_ref[s] = sums * (1.0 / sums[6:7])

    for i in range(HALF):
        first(i, i)

    def one_group(g, carry):
        base = g * (2 * HALF)
        after = jnp.minimum(base + 2 * HALF, segs - HALF)
        for i in range(HALF):
            second(base + i, i)
            first(base + HALF + i, HALF + i)
        for i in range(HALF):
            second(base + HALF + i, HALF + i)
            first(after + i, i)
        return carry

    lax.fori_loop(0, segs // (2 * HALF), one_group, 0)


def sec_kernel(
    capacity, slots_ref, fetched_ref, points_ref, other_ref, out_ref, both_ref, lhs_ref, left_ref
):
    segs = points_ref.shape[0]
    out_ref[...] = jnp.zeros_like(out_ref)

    def first(s, i):
        stage_a(capacity, s, slots_ref[s], fetched_ref, points_ref, both_ref, lhs_ref, i)

    def second(s, i):
        sums = sums_of(both_ref, lhs_ref, i)
        inverse = 1.0 / sums[6:7]
        gap = (points_ref[s, 5:6] * inverse) * (sums * inverse - other_ref[s])
        high = gap.astype(jnp.bfloat16).astype(jnp.float32)
        left_ref[i] = jnp.concatenate([high, gap - high], axis=0).astype(jnp.bfloat16)

    def third(s, i):
        slot = slots_ref[s]
        result = lax.dot_general(
            left_ref[i], both_ref[i], (((1,), (1,)), ((), ())), preferred_element_type=jnp.float32
        )
        half = result.shape[1] // 2
        result = result[:8] + result[8:]
        result = result[:, :half] + result[:, half:]
        base = (slot // capacity) * (3 * capacity) + slot % capacity
        out_ref[pl.ds(base, 3, stride=capacity), :] = result[3:6]

    for i in range(HALF):
        first(i, i)

    def one_group(g, carry):
        base = g * (2 * HALF)
        after = jnp.minimum(base + 2 * HALF, segs - HALF)
        for i in range(HALF):
            second(base + i, i)
            first(base + HALF + i, HALF + i)
        for i in range(HALF):
            third(base + i, i)
            second(base + HALF + i, HALF + i)
        for i in range(HALF):
            third(base + HALF + i, HALF + i)
            first(after + i, i)
        return carry

    lax.fori_loop(0, segs // (2 * HALF), one_group, 0)


def body(node_coords, node_disp, qpoints, qweights, qcount, sec_block, pri_block):
    devices = lax.axis_size("gx") * lax.axis_size("gy")
    blocks = node_coords.shape[0]
    nodes = node_coords.shape[2]
    segs = qpoints.shape[0]
    quad = qpoints.shape[2]
    slots = 2 * segs
    cap = slots // devices
    f32 = jnp.float32
    smem = pl.BlockSpec(memory_space=pltpu.SMEM)
    vmem = pl.BlockSpec(memory_space=pltpu.VMEM)

    def exchange(value):
        return lax.all_to_all(value, AXES, split_axis=0, concat_axis=0, tiled=True)

    sec_slots, sec_request = routing(sec_block, blocks, cap, slots)
    pri_slots, pri_request = routing(pri_block, blocks, cap, slots)
    requests = jnp.concatenate(
        [sec_request.reshape(devices, cap), pri_request.reshape(devices, cap)], axis=1
    )
    received = exchange(requests)
    sec_ids = received[:, :cap].reshape(slots)
    pri_ids = received[:, cap:].reshape(slots)

    xc = jnp.transpose(node_coords, (1, 0, 2)).reshape(3 * blocks, nodes)
    xu = jnp.transpose(node_disp, (1, 0, 2)).reshape(3 * blocks, nodes)
    gather = pl.pallas_call(
        functools.partial(gather_kernel, devices, cap, blocks),
        out_shape=jax.ShapeDtypeStruct((devices * 6 * cap, nodes), f32),
        in_specs=[smem, vmem, vmem],
        out_specs=vmem,
    )
    pri_in = exchange(gather(pri_ids, xc, xu).reshape(devices, 6 * cap, nodes)).reshape(-1, nodes)
    sec_in = exchange(gather(sec_ids, xc, xu).reshape(devices, 6 * cap, nodes)).reshape(-1, nodes)

    live = jnp.arange(quad, dtype=jnp.int32)[None, :] < qcount[:, None]
    weights = jnp.where(live, qweights, jnp.zeros_like(qweights))
    qx, qy, qz = qpoints[:, 0], qpoints[:, 1], qpoints[:, 2]
    ones = jnp.ones_like(qx)
    zeros = jnp.zeros_like(qx)
    square = 1.0 + 2.0 * (qx * qx + qy * qy + qz * qz)
    points = jnp.stack([qx, qy, qz, ones, square, weights, zeros, zeros], axis=1)

    scratch = [
        pltpu.VMEM((2 * HALF, 2 * nodes, quad), jnp.bfloat16),
        pltpu.VMEM((2 * HALF, 16, 2 * nodes), jnp.bfloat16),
    ]
    other = pl.pallas_call(
        functools.partial(pri_kernel, cap),
        out_shape=jax.ShapeDtypeStruct((segs, 8, quad), f32),
        in_specs=[smem, vmem, vmem],
        out_specs=vmem,
        scratch_shapes=scratch,
    )(pri_slots, pri_in, points)
    parcels = pl.pallas_call(
        functools.partial(sec_kernel, cap),
        out_shape=jax.ShapeDtypeStruct((devices * 3 * cap, nodes), f32),
        in_specs=[smem, vmem, vmem, vmem],
        out_specs=vmem,
        scratch_shapes=scratch + [pltpu.VMEM((2 * HALF, 16, quad), jnp.bfloat16)],
    )(sec_slots, sec_in, points, other)
    incoming = exchange(parcels.reshape(devices, 3, cap, nodes))
    select = (jnp.arange(blocks, dtype=jnp.int32)[:, None] == sec_ids[None, :]).astype(f32)
    incoming = jnp.transpose(incoming, (0, 2, 1, 3)).reshape(slots, 3, nodes)
    return jnp.einsum("bp,pcn->bcn", select, incoming, precision=lax.Precision.HIGHEST)


def solution(mesh):
    split3 = P(AXES, None, None)
    placed = (split3, split3, split3, P(AXES, None), P(AXES), P(AXES), P(AXES))
    return jax.shard_map(body, mesh=mesh, in_specs=placed, out_specs=split3, check_vma=False)
```

```python
import functools
import jax
import jax.numpy as jnp
from jax import lax
from jax.experimental import pallas as pl
from jax.experimental.pallas import tpu as pltpu
from jax.sharding import PartitionSpec as P

AXES = ("gx", "gy")
HALF = 8


def routing(block_ids, blocks_dev, capacity, slot_count):
    owners = block_ids // blocks_dev
    local_ids = block_ids % blocks_dev
    positions = jnp.arange(block_ids.shape[0], dtype=jnp.int32)
    same_owner = (owners[:, None] == owners[None, :]) & (positions[:, None] > positions[None, :])
    ranks = jnp.sum(same_owner.astype(jnp.int32), axis=1)
    slot_ids = owners * capacity + ranks
    matches = slot_ids[:, None] == jnp.arange(slot_count, dtype=jnp.int32)[None, :]
    request = jnp.sum(jnp.where(matches, local_ids[:, None], 0), axis=0)
    return (slot_ids, request)


def gather_kernel(devices, capacity, blocks, first, ids_ref, xc_ref, xu_ref, out_ref):
    if first:
        parts = [(1, rank, rank, capacity) for rank in range(capacity)]
        parts.append((0, 0, 6 * capacity, 1))
    else:
        parts = [(0, rank, rank - 1, capacity - 1) for rank in range(1, capacity)]
    rows = 6 * len(parts)

    def one_device(dev, carry):
        for side, rank, start, step in parts:
            local = ids_ref[dev * (2 * capacity) + side * capacity + rank]
            base = dev * rows + start
            out_ref[pl.ds(base, 3, stride=step), :] = xc_ref[pl.ds(local, 3, stride=blocks), :]
            out_ref[pl.ds(base + 3 * step, 3, stride=step), :] = xu_ref[
                pl.ds(local, 3, stride=blocks), :
            ]
        return carry

    lax.fori_loop(0, devices, one_device, 0, unroll=4)


def pack_kernel(points_ref, out_ref):
    rows = 8
    segs = points_ref.shape[1]
    out_ref[...] = jnp.zeros_like(out_ref)

    def one_block(b, carry):
        here = pl.ds(pl.multiple_of(b * rows, rows), rows)
        x, y, z = points_ref[0, here], points_ref[1, here], points_ref[2, here]
        square = 1.0 + 2.0 * (x * x + y * y + z * z)
        for row, value in enumerate((x, y, z, jnp.ones_like(x), square)):
            for half in range(x.shape[1] // 128):
                lanes = slice(half * 128, half * 128 + 128)
                out_ref[half, pl.ds(b * rows * rows + row, rows, stride=rows), :] = value[:, lanes]
        return carry

    lax.fori_loop(0, segs // rows, one_block, 0, unroll=2)


def pieces(value):
    first = value.astype(jnp.bfloat16).astype(jnp.float32)
    rest = value - first
    second = rest.astype(jnp.bfloat16).astype(jnp.float32)
    return (first, second, rest - second)


def node_side(fetched_ref, start, step):
    raw = fetched_ref[pl.ds(start, 6, stride=step), :]
    raw = jnp.concatenate([raw, jnp.zeros((2, raw.shape[1]), jnp.float32)], axis=0)
    row = lax.broadcasted_iota(jnp.int32, raw.shape, 0)
    coord = jnp.where(row < 3, raw, 0.0)
    square = 2.0 * jnp.sum(coord * coord, axis=0, keepdims=True)
    extended = jnp.where(row == 3, square, jnp.where(row == 4, 1.0, -4.0 * coord))
    a, b, c = pieces(extended)
    stacked = jnp.concatenate([a, a, b, b, a, c], axis=0)
    disp = jnp.where(row < 3, 0.0, jnp.where(row == 6, 1.0, raw))
    high = disp.astype(jnp.bfloat16).astype(jnp.float32)
    lhs = jnp.concatenate([high, disp - high], axis=0)
    lhs = jnp.concatenate([lhs, lhs], axis=1).astype(jnp.bfloat16)
    return stacked.T.astype(jnp.bfloat16), lhs


def points_of(points_ref, s):
    here = pl.ds(pl.multiple_of(s * 8, 8), 8)
    return jnp.concatenate([points_ref[h, here] for h in range(points_ref.shape[0])], axis=1)


def point_side(points):
    a, b, c = pieces(points)
    return jnp.concatenate([a, b, a, b, c, a], axis=0).astype(jnp.bfloat16)


def kernel_values(node_op, point_op):
    dist = jnp.dot(node_op, point_op, preferred_element_type=jnp.float32)
    value = 1.0 / dist
    high = value.astype(jnp.bfloat16)
    low = (value - high.astype(jnp.float32)).astype(jnp.bfloat16)
    return jnp.concatenate([high, low], axis=0)


def stage_a(s, start, step, fetched_ref, points_ref, both_ref, lhs_ref, i):
    node_op, lhs = node_side(fetched_ref, start, step)
    lhs_ref[i] = lhs
    both_ref[i] = kernel_values(node_op, point_side(points_of(points_ref, s)))


def sums_of(both_ref, lhs_ref, i):
    sums = jnp.dot(lhs_ref[i], both_ref[i], preferred_element_type=jnp.float32)
    return sums[:8] + sums[8:]


def pri_kernel(capacity, slots_ref, fetched_ref, points_ref, out_ref, both_ref, lhs_ref):
    segs = slots_ref.shape[0]

    def first(s, i):
        slot = slots_ref[s]
        start = (slot // capacity) * (6 * capacity + 6) + slot % capacity
        stage_a(s, start, capacity, fetched_ref, points_ref, both_ref, lhs_ref, i)

    def second(s, i):
        sums = sums_of(both_ref, lhs_ref, i)
        out_ref[s] = sums * (1.0 / sums[6:7])

    for i in range(HALF):
        first(i, i)

    def one_group(g, carry):
        base = g * (2 * HALF)
        after = jnp.minimum(base + 2 * HALF, segs - HALF)
        for i in range(HALF):
            second(base + i, i)
            first(base + HALF + i, HALF + i)
        for i in range(HALF):
            second(base + HALF + i, HALF + i)
            first(after + i, i)
        return carry

    lax.fori_loop(0, segs // (2 * HALF), one_group, 0)


def sec_kernel(early, capacity, *refs):
    slots_ref, count_ref, order_ref, early_ref, fetched_ref, points_ref, weights_ref, other_ref = refs[:8]
    if early:
        out_ref, both_ref, lhs_ref, left_ref = refs[8:]
        out_ref[...] = jnp.zeros_like(out_ref)
        low, high_end = 0, early_ref[0]
    else:
        before_ref, out_ref, both_ref, lhs_ref, left_ref = refs[8:]
        out_ref[...] = before_ref[...]
        low, high_end = early_ref[0], slots_ref.shape[0]

    def segment(place):
        return order_ref[jnp.minimum(low + place, high_end - 1)]

    def first(place, i):
        s = segment(place)
        slot = slots_ref[s]
        dev, rank = slot // capacity, slot % capacity
        if early:
            start, step = dev * (6 * capacity + 6) + 6 * capacity, 1
        else:
            start, step = dev * (6 * capacity - 6) + (rank - 1), capacity - 1
        stage_a(s, start, step, fetched_ref, points_ref, both_ref, lhs_ref, i)

    def second(place, i):
        s = segment(place)
        sums = sums_of(both_ref, lhs_ref, i)
        inverse = 1.0 / sums[6:7]
        weights = weights_ref[pl.ds(s, 1), :]
        position = lax.broadcasted_iota(jnp.int32, weights.shape, 1)
        weights = jnp.where(position < count_ref[s], weights, 0.0)
        gap = (weights * inverse) * (sums * inverse - other_ref[s])
        high = gap.astype(jnp.bfloat16).astype(jnp.float32)
        left_ref[i] = jnp.concatenate([high, gap - high], axis=0).astype(jnp.bfloat16)

    def third(place, i):
        slot = slots_ref[segment(place)]
        result = lax.dot_general(
            left_ref[i], both_ref[i], (((1,), (1,)), ((), ())), preferred_element_type=jnp.float32
        )
        half = result.shape[1] // 2
        result = result[:8] + result[8:]
        result = result[:, :half] + result[:, half:]
        base = (slot // capacity) * (3 * capacity) + slot % capacity
        out_ref[pl.ds(base, 3, stride=capacity), :] = result[3:6]

    for i in range(HALF):
        first(i, i)

    def one_group(g, carry):
        base = g * (2 * HALF)
        for i in range(HALF):
            second(base + i, i)
            first(base + HALF + i, HALF + i)
        for i in range(HALF):
            third(base + i, i)
            second(base + HALF + i, HALF + i)
        for i in range(HALF):
            third(base + HALF + i, HALF + i)
            first(base + 2 * HALF + i, i)
        return carry

    lax.fori_loop(0, (high_end - low + 2 * HALF - 1) // (2 * HALF), one_group, 0)


def body(node_coords, node_disp, qpoints, qweights, qcount, sec_block, pri_block):
    devices = lax.axis_size("gx") * lax.axis_size("gy")
    blocks = node_coords.shape[0]
    nodes = node_coords.shape[2]
    segs = qpoints.shape[0]
    quad = qpoints.shape[2]
    slots = 2 * segs
    cap = slots // devices
    f32 = jnp.float32
    smem = pl.BlockSpec(memory_space=pltpu.SMEM)
    vmem = pl.BlockSpec(memory_space=pltpu.VMEM)

    def exchange(value):
        return lax.all_to_all(value, AXES, split_axis=0, concat_axis=0, tiled=True)

    sec_slots, sec_request = routing(sec_block, blocks, cap, slots)
    pri_slots, pri_request = routing(pri_block, blocks, cap, slots)
    requests = jnp.concatenate(
        [sec_request.reshape(devices, cap), pri_request.reshape(devices, cap)], axis=1
    )
    received = exchange(requests)
    sec_ids = received[:, :cap].reshape(slots)
    ids = received.reshape(2 * slots)

    is_early = sec_slots % cap == 0
    early = jnp.sum(is_early.astype(jnp.int32))
    here = jnp.arange(segs, dtype=jnp.int32)
    same = (is_early[:, None] == is_early[None, :]) & (here[:, None] > here[None, :])
    place = jnp.sum(same.astype(jnp.int32), axis=1) + jnp.where(is_early, 0, early)
    order = jnp.sum(jnp.where(place[:, None] == here[None, :], here[:, None], 0), axis=0)
    early = early.reshape(1)

    xc = jnp.transpose(node_coords, (1, 0, 2)).reshape(3 * blocks, nodes)
    xu = jnp.transpose(node_disp, (1, 0, 2)).reshape(3 * blocks, nodes)
    scratch = [
        pltpu.VMEM((2 * HALF, 2 * nodes, quad), jnp.bfloat16),
        pltpu.VMEM((2 * HALF, 16, 2 * nodes), jnp.bfloat16),
    ]

    limit = pltpu.CompilerParams(vmem_limit_bytes=16 * 1024 * 1024)

    def near(value):
        return pltpu.with_memory_space_constraint(value, pltpu.VMEM)

    def gather(first, rows):
        return pl.pallas_call(
            functools.partial(gather_kernel, devices, cap, blocks, first),
            out_shape=jax.ShapeDtypeStruct((devices * rows, nodes), f32),
            in_specs=[smem, vmem, vmem],
            out_specs=vmem,
            compiler_params=limit,
        )(ids, xc, xu).reshape(devices, rows // 2, 2, nodes)

    out1 = gather(True, 6 * cap + 6)
    out2 = gather(False, 6 * cap - 6)
    in1 = near(exchange(out1).reshape(-1, nodes))
    in2 = near(exchange(out2).reshape(-1, nodes))
    points = pl.pallas_call(
        pack_kernel,
        out_shape=pltpu.VMEM((quad // 128, segs * 8, 128), f32),
        in_specs=[vmem],
        out_specs=vmem,
        compiler_params=limit,
    )(jnp.transpose(qpoints, (1, 0, 2)))
    points = near(points)
    other = pl.pallas_call(
        functools.partial(pri_kernel, cap),
        out_shape=pltpu.VMEM((segs, 8, quad), f32),
        in_specs=[smem, vmem, vmem],
        out_specs=vmem,
        compiler_params=limit,
        scratch_shapes=scratch,
    )(pri_slots, in1, points)

    def secondary(early_part, *args):
        return pl.pallas_call(
            functools.partial(sec_kernel, early_part, cap),
            out_shape=pltpu.VMEM((devices * 3 * cap, nodes), f32),
            in_specs=[smem] * 4 + [vmem] * (len(args) - 4),
            out_specs=vmem,
            compiler_params=limit,
            scratch_shapes=scratch + [pltpu.VMEM((2 * HALF, 16, quad), jnp.bfloat16)],
        )(*args)

    other = near(other)
    parcels = near(secondary(True, sec_slots, qcount, order, early, in1, points, qweights, other))
    parcels = secondary(
        False, sec_slots, qcount, order, early, in2, points, qweights, other, parcels
    )
    incoming = exchange(parcels.reshape(devices, 3, cap, nodes))
    select = (jnp.arange(blocks, dtype=jnp.int32)[:, None] == sec_ids[None, :]).astype(f32)
    incoming = jnp.transpose(incoming, (0, 2, 1, 3)).reshape(slots, 3, nodes)
    return jnp.einsum("bp,pcn->bcn", select, incoming, precision=lax.Precision.HIGHEST)


def solution(mesh):
    split3 = P(AXES, None, None)
    placed = (split3, split3, split3, P(AXES, None), P(AXES), P(AXES), P(AXES))
    return jax.shard_map(body, mesh=mesh, in_specs=placed, out_specs=split3, check_vma=False)
```

```python
import functools
import jax
import jax.numpy as jnp
from jax import lax
from jax.experimental import pallas as pl
from jax.experimental.pallas import tpu as pltpu
from jax.sharding import PartitionSpec as P

AXES = ("gx", "gy")
HALF = 8
WIDE = 16


def routing(block_ids, blocks_dev, capacity, slot_count):
    owners = block_ids // blocks_dev
    local_ids = block_ids % blocks_dev
    positions = jnp.arange(block_ids.shape[0], dtype=jnp.int32)
    same_owner = (owners[:, None] == owners[None, :]) & (positions[:, None] > positions[None, :])
    ranks = jnp.sum(same_owner.astype(jnp.int32), axis=1)
    slot_ids = owners * capacity + ranks
    matches = slot_ids[:, None] == jnp.arange(slot_count, dtype=jnp.int32)[None, :]
    request = jnp.sum(jnp.where(matches, local_ids[:, None], 0), axis=0)
    return (slot_ids, request)


def table_kernel(xc_ref, xu_ref, out_ref):
    half = xc_ref.shape[0]
    out_ref[:half] = xc_ref[...]
    out_ref[half:] = xu_ref[...]


def gather_kernel(devices, capacity, blocks, first, ids_ref, table_ref, out_ref):
    if first:
        parts = [(1, rank, rank, capacity) for rank in range(capacity)]
        parts.append((0, 0, 6 * capacity, 1))
    else:
        parts = [(0, rank, rank - 1, capacity - 1) for rank in range(1, capacity)]
    rows = 6 * len(parts)

    def one_device(dev, carry):
        for side, rank, start, step in parts:
            local = ids_ref[dev * (2 * capacity) + side * capacity + rank]
            out_ref[pl.ds(dev * rows + start, 6, stride=step), :] = table_ref[
                pl.ds(local, 6, stride=blocks), :
            ]
        return carry

    lax.fori_loop(0, devices, one_device, 0, unroll=4)


def pack_kernel(points_ref, out_ref):
    rows = 8
    segs = points_ref.shape[1]
    out_ref[...] = jnp.zeros_like(out_ref)

    def one_block(b, carry):
        here = pl.ds(pl.multiple_of(b * rows, rows), rows)
        x, y, z = points_ref[0, here], points_ref[1, here], points_ref[2, here]
        square = 1.0 + 2.0 * (x * x + y * y + z * z)
        for row, value in enumerate((x, y, z, jnp.ones_like(x), square)):
            for half in range(x.shape[1] // 128):
                lanes = slice(half * 128, half * 128 + 128)
                out_ref[half, pl.ds(b * rows * rows + row, rows, stride=rows), :] = value[:, lanes]
        return carry

    lax.fori_loop(0, segs // rows, one_block, 0, unroll=2)


def pieces(value):
    first = value.astype(jnp.bfloat16).astype(jnp.float32)
    rest = value - first
    second = rest.astype(jnp.bfloat16).astype(jnp.float32)
    return (first, second, rest - second)


def node_side(fetched_ref, start, step):
    raw = fetched_ref[pl.ds(start, 6, stride=step), :]
    raw = jnp.concatenate([raw, jnp.zeros((2, raw.shape[1]), jnp.float32)], axis=0)
    row = lax.broadcasted_iota(jnp.int32, raw.shape, 0)
    coord = jnp.where(row < 3, raw, 0.0)
    square = 2.0 * jnp.sum(coord * coord, axis=0, keepdims=True)
    extended = jnp.where(row == 3, square, jnp.where(row == 4, 1.0, -4.0 * coord))
    a, b, c = pieces(extended)
    stacked = jnp.concatenate([a, a, b, b, a, c], axis=0)
    disp = jnp.where(row < 3, 0.0, jnp.where(row == 6, 1.0, raw))
    high = disp.astype(jnp.bfloat16).astype(jnp.float32)
    lhs = jnp.concatenate([high, disp - high], axis=0)
    lhs = jnp.concatenate([lhs, lhs], axis=1).astype(jnp.bfloat16)
    return stacked.T.astype(jnp.bfloat16), lhs


def points_of(points_ref, s):
    here = pl.ds(pl.multiple_of(s * 8, 8), 8)
    return jnp.concatenate([points_ref[h, here] for h in range(points_ref.shape[0])], axis=1)


def point_side(points):
    a, b, c = pieces(points)
    return jnp.concatenate([a, b, a, b, c, a], axis=0).astype(jnp.bfloat16)


def kernel_values(node_op, point_op):
    dist = jnp.dot(node_op, point_op, preferred_element_type=jnp.float32)
    value = 1.0 / dist
    high = value.astype(jnp.bfloat16)
    low = (value - high.astype(jnp.float32)).astype(jnp.bfloat16)
    return jnp.concatenate([high, low], axis=0)


def stage_a(s, start, step, fetched_ref, points_ref, both_ref, lhs_ref, i):
    node_op, lhs = node_side(fetched_ref, start, step)
    lhs_ref[i] = lhs
    both_ref[i] = kernel_values(node_op, point_side(points_of(points_ref, s)))


def sums_of(both_ref, lhs_ref, i):
    sums = jnp.dot(lhs_ref[i], both_ref[i], preferred_element_type=jnp.float32)
    return sums[:8] + sums[8:]


def pri_kernel(capacity, slots_ref, fetched_ref, points_ref, out_ref, both_ref, lhs_ref):
    segs = slots_ref.shape[0]

    def first(s, i):
        slot = slots_ref[s]
        start = (slot // capacity) * (6 * capacity + 6) + slot % capacity
        stage_a(s, start, capacity, fetched_ref, points_ref, both_ref, lhs_ref, i)

    def second(s, i):
        sums = sums_of(both_ref, lhs_ref, i)
        out_ref[s] = sums * (1.0 / sums[6:7])

    for i in range(WIDE):
        first(i, i)

    def one_group(g, carry):
        base = g * (2 * WIDE)
        after = jnp.minimum(base + 2 * WIDE, segs - WIDE)
        for i in range(WIDE):
            second(base + i, i)
            first(base + WIDE + i, WIDE + i)
        for i in range(WIDE):
            second(base + WIDE + i, WIDE + i)
            first(after + i, i)
        return carry

    lax.fori_loop(0, segs // (2 * WIDE), one_group, 0)


def sec_kernel(early, capacity, *refs):
    slots_ref, count_ref, order_ref, early_ref, fetched_ref, points_ref, weights_ref = refs[:7]
    if early:
        far_ref, out_ref, both_ref, lhs_ref, left_ref, other_ref, sems = refs[7:]
        out_ref[...] = jnp.zeros_like(out_ref)
        low, high_end = 0, early_ref[0]
        copies = []
    else:
        far_ref, before_ref, out_ref, both_ref, lhs_ref, left_ref, other_ref, sems = refs[7:]
        low, high_end = early_ref[0], slots_ref.shape[0]
        copies = [pltpu.make_async_copy(before_ref, out_ref, sems.at[1])]
    copies.append(pltpu.make_async_copy(far_ref, other_ref, sems.at[0]))
    for copy in copies:
        copy.start()

    def segment(place):
        return order_ref[jnp.minimum(low + place, high_end - 1)]

    def first(place, i):
        s = segment(place)
        slot = slots_ref[s]
        dev, rank = slot // capacity, slot % capacity
        if early:
            start, step = dev * (6 * capacity + 6) + 6 * capacity, 1
        else:
            start, step = dev * (6 * capacity - 6) + (rank - 1), capacity - 1
        stage_a(s, start, step, fetched_ref, points_ref, both_ref, lhs_ref, i)

    def second(place, i):
        s = segment(place)
        sums = sums_of(both_ref, lhs_ref, i)
        inverse = 1.0 / sums[6:7]
        weights = weights_ref[pl.ds(s, 1), :]
        position = lax.broadcasted_iota(jnp.int32, weights.shape, 1)
        weights = jnp.where(position < count_ref[s], weights, 0.0)
        gap = (weights * inverse) * (sums * inverse - other_ref[s])
        high = gap.astype(jnp.bfloat16).astype(jnp.float32)
        left_ref[i] = jnp.concatenate([high, gap - high], axis=0).astype(jnp.bfloat16)

    def third(place, i):
        slot = slots_ref[segment(place)]
        left, both = left_ref[i], both_ref[i]
        half = both.shape[0] // 2
        if i % 2 == 0:
            result = lax.dot_general(
                left, both, (((1,), (1,)), ((), ())), preferred_element_type=jnp.float32
            )
            result = result[:8] + result[8:]
            result = result[:, :half] + result[:, half:]
        else:
            result = lax.dot_general(
                both, left, (((1,), (1,)), ((), ())), preferred_element_type=jnp.float32
            )
            result = (result[:half] + result[half:]).T
            result = result[:8] + result[8:]
        base = (slot // capacity) * (3 * capacity) + slot % capacity
        out_ref[pl.ds(base, 3, stride=capacity), :] = result[3:6]

    for i in range(HALF):
        first(i, i)
    for copy in copies:
        copy.wait()

    def one_group(g, carry):
        base = g * (2 * HALF)
        for i in range(HALF):
            second(base + i, i)
            first(base + HALF + i, HALF + i)
        for i in range(HALF):
            third(base + i, i)
            second(base + HALF + i, HALF + i)
        for i in range(HALF):
            third(base + HALF + i, HALF + i)
            first(base + 2 * HALF + i, i)
        return carry

    lax.fori_loop(0, (high_end - low + 2 * HALF - 1) // (2 * HALF), one_group, 0)


def body(node_coords, node_disp, qpoints, qweights, qcount, sec_block, pri_block):
    devices = lax.axis_size("gx") * lax.axis_size("gy")
    blocks = node_coords.shape[0]
    nodes = node_coords.shape[2]
    segs = qpoints.shape[0]
    quad = qpoints.shape[2]
    slots = 2 * segs
    cap = slots // devices
    f32 = jnp.float32
    smem = pl.BlockSpec(memory_space=pltpu.SMEM)
    vmem = pl.BlockSpec(memory_space=pltpu.VMEM)

    limit = pltpu.CompilerParams(vmem_limit_bytes=16 * 1024 * 1024)

    def near(value):
        return pltpu.with_memory_space_constraint(value, pltpu.VMEM)

    def far(value):
        return pltpu.with_memory_space_constraint(value, pltpu.HBM)

    def exchange(value):
        return lax.all_to_all(value, AXES, split_axis=0, concat_axis=0, tiled=True)

    sec_slots, sec_request = routing(sec_block, blocks, cap, slots)
    pri_slots, pri_request = routing(pri_block, blocks, cap, slots)
    xc = jnp.transpose(node_coords, (1, 0, 2)).reshape(3 * blocks, nodes)
    xu = jnp.transpose(node_disp, (1, 0, 2)).reshape(3 * blocks, nodes)
    hbm = pl.BlockSpec(memory_space=pltpu.HBM)
    table = pl.pallas_call(
        table_kernel,
        out_shape=pltpu.VMEM((6 * blocks, nodes), f32),
        in_specs=[vmem, vmem],
        out_specs=vmem,
        compiler_params=limit,
    )(far(xc), far(xu))
    requests = jnp.concatenate(
        [sec_request.reshape(devices, cap), pri_request.reshape(devices, cap)], axis=1
    )
    received = exchange(requests)
    sec_ids = received[:, :cap].reshape(slots)
    ids = received.reshape(2 * slots)

    is_early = sec_slots % cap == 0
    early = jnp.sum(is_early.astype(jnp.int32))
    here = jnp.arange(segs, dtype=jnp.int32)
    same = (is_early[:, None] == is_early[None, :]) & (here[:, None] > here[None, :])
    place = jnp.sum(same.astype(jnp.int32), axis=1) + jnp.where(is_early, 0, early)
    order = jnp.sum(jnp.where(place[:, None] == here[None, :], here[:, None], 0), axis=0)
    early = early.reshape(1)

    def scratch(count):
        return [
            pltpu.VMEM((2 * count, 2 * nodes, quad), jnp.bfloat16),
            pltpu.VMEM((2 * count, 16, 2 * nodes), jnp.bfloat16),
        ]

    def gather(first, rows):
        return pl.pallas_call(
            functools.partial(gather_kernel, devices, cap, blocks, first),
            out_shape=pltpu.HBM((devices * rows, nodes), f32),
            in_specs=[smem, vmem],
            out_specs=vmem,
            compiler_params=limit,
        )(ids, near(table)).reshape(devices, rows // 2, 2, nodes)

    out1 = gather(True, 6 * cap + 6)
    out2 = gather(False, 6 * cap - 6)
    in1 = near(exchange(out1).reshape(-1, nodes))
    in2 = near(exchange(out2).reshape(-1, nodes))
    points = pl.pallas_call(
        pack_kernel,
        out_shape=pltpu.VMEM((quad // 128, segs * 8, 128), f32),
        in_specs=[vmem],
        out_specs=vmem,
        compiler_params=limit,
    )(jnp.transpose(qpoints, (1, 0, 2)))
    points = near(points)
    other = pl.pallas_call(
        functools.partial(pri_kernel, cap),
        out_shape=pltpu.HBM((segs, 8, quad), f32),
        in_specs=[smem, vmem, vmem],
        out_specs=vmem,
        compiler_params=limit,
        scratch_shapes=scratch(WIDE),
    )(pri_slots, in1, points)

    def secondary(early_part, *args):
        return pl.pallas_call(
            functools.partial(sec_kernel, early_part, cap),
            out_shape=pltpu.HBM((devices * 3 * cap, nodes), f32),
            in_specs=[smem] * 4 + [vmem] * 3 + [hbm] * (len(args) - 7),
            out_specs=vmem,
            compiler_params=limit,
            scratch_shapes=scratch(HALF)
            + [
                pltpu.VMEM((2 * HALF, 16, quad), jnp.bfloat16),
                pltpu.VMEM((segs, 8, quad), f32),
                pltpu.SemaphoreType.DMA((2,)),
            ],
        )(*args)

    other = far(other)
    parcels = secondary(True, sec_slots, qcount, order, early, in1, points, qweights, other)
    parcels = far(parcels)
    parcels = secondary(
        False, sec_slots, qcount, order, early, in2, points, qweights, other, parcels
    )
    incoming = exchange(parcels.reshape(devices, 3, cap, nodes))
    select = (jnp.arange(blocks, dtype=jnp.int32)[:, None] == sec_ids[None, :]).astype(f32)
    incoming = jnp.transpose(incoming, (0, 2, 1, 3)).reshape(slots, 3, nodes)
    return jnp.einsum("bp,pcn->bcn", select, incoming, precision=lax.Precision.HIGHEST)


def solution(mesh):
    split3 = P(AXES, None, None)
    placed = (split3, split3, split3, P(AXES, None), P(AXES), P(AXES), P(AXES))
    return jax.shard_map(body, mesh=mesh, in_specs=placed, out_specs=split3, check_vma=False)
```

```python
import functools
import jax
import jax.numpy as jnp
from jax import lax
from jax.experimental import pallas as pl
from jax.experimental.pallas import tpu as pltpu
from jax.sharding import PartitionSpec as P

AXES = ("gx", "gy")
HALF = 8
WIDE = 16


def strict_upper(size):
    row = lax.broadcasted_iota(jnp.int32, (size, size), 0)
    column = lax.broadcasted_iota(jnp.int32, (size, size), 1)
    return jnp.where(row < column, 1.0, 0.0).astype(jnp.bfloat16)


def dot_last(left, right):
    return lax.dot_general(
        left, right, (((1,), (1,)), ((), ())), preferred_element_type=jnp.float32
    )


def plan_kernel(devices, capacity, blocks, sec_ref, pri_ref, plan_ref, request_ref):
    segs = sec_ref.shape[1]
    upper = strict_upper(segs)
    device = lax.broadcasted_iota(jnp.int32, (devices, segs), 0).astype(jnp.float32)
    column = lax.broadcasted_iota(jnp.int32, (request_ref.shape[1], segs), 0).astype(jnp.float32)
    request = jnp.zeros(request_ref.shape, jnp.float32)
    routes = []
    for side, ref in enumerate((sec_ref, pri_ref)):
        ids = ref[...].astype(jnp.float32)
        owner = jnp.floor((ids + 0.5) * (1.0 / blocks))
        local = ids - owner * blocks
        mine = jnp.where(device == owner, 1.0, 0.0)
        narrow = mine.astype(jnp.bfloat16)
        before = jnp.dot(narrow, upper, preferred_element_type=jnp.float32)
        rank = jnp.sum(mine * before, axis=0, keepdims=True)
        coarse = jnp.floor(local * (1.0 / 16.0)) * 16.0
        here = column == rank + side * capacity
        for part in (coarse, local - coarse):
            request += dot_last(narrow, jnp.where(here, part, 0.0).astype(jnp.bfloat16))
        routes.append((owner, rank))
    request_ref[...] = request

    (sec_owner, sec_rank), (pri_owner, pri_rank) = routes
    early = jnp.where(sec_rank == 0.0, 1.0, 0.0)
    spread = jnp.broadcast_to(early, (16, segs)).astype(jnp.bfloat16)
    ahead = jnp.dot(spread, upper, preferred_element_type=jnp.float32)[:1]
    count = jnp.sum(early, axis=1, keepdims=True)
    number = lax.broadcasted_iota(jnp.int32, (1, segs), 1).astype(jnp.float32)
    place = jnp.where(sec_rank == 0.0, ahead, count + number - ahead)
    target = lax.broadcasted_iota(jnp.int32, (segs, segs), 0).astype(jnp.float32)
    moved = jnp.where(target == place, 1.0, 0.0).astype(jnp.bfloat16)
    row = lax.broadcasted_iota(jnp.int32, (16, segs), 0)
    values = jnp.where(row == 0, number, jnp.where(row == 1, sec_owner, sec_rank))
    values = dot_last(values.astype(jnp.bfloat16), moved)
    seg, dev, rank = values[0:1], values[1:2], values[2:3]
    start = jnp.where(
        rank == 0.0,
        dev * (6 * capacity + 6) + 6 * capacity,
        dev * (6 * capacity - 6) + (rank - 1.0),
    )
    rows = (
        pri_owner * (6 * capacity + 6) + pri_rank,
        seg,
        start,
        dev * (3 * capacity) + rank,
        jnp.broadcast_to(count, (1, segs)),
    )
    plan_ref[...] = jnp.zeros_like(plan_ref)
    for i, value in enumerate(rows):
        plan_ref[i : i + 1, :] = value.astype(jnp.int32)


def table_kernel(xc_ref, xu_ref, out_ref):
    blocks = xc_ref.shape[0] // 3

    def one_block(b, carry):
        for half, ref in enumerate((xc_ref, xu_ref)):
            for c in range(3):
                here = pl.ds(pl.multiple_of(c * blocks + b * 8, 8), 8)
                out_ref[pl.ds(b * 64 + 3 * half + c, 8, stride=8), :] = ref[here, :]
        return carry

    lax.fori_loop(0, blocks // 8, one_block, 0, unroll=4)


def gather_kernel(devices, capacity, first, ids_ref, table_ref, out_ref, turned, local_ref, sem):
    turned[...] = ids_ref[...].T[: 2 * capacity].astype(jnp.int32)
    copy = pltpu.make_async_copy(turned, local_ref, sem)
    copy.start()
    copy.wait()
    if first:
        parts = [(1, rank, rank, capacity) for rank in range(capacity)]
        parts.append((0, 0, 6 * capacity, 1))
    else:
        parts = [(0, rank, rank - 1, capacity - 1) for rank in range(1, capacity)]
    rows = 6 * len(parts)

    def one_device(dev, carry):
        for side, rank, start, step in parts:
            local = local_ref[side * capacity + rank, dev]
            patch = table_ref[pl.ds(pl.multiple_of(local * 8, 8), 8), :]
            out_ref[pl.ds(dev * rows + start, 6, stride=step), :] = patch[:6]
        return carry

    lax.fori_loop(0, devices, one_device, 0, unroll=4)


def pack_kernel(points_ref, out_ref):
    rows = 8
    segs = points_ref.shape[1]
    out_ref[...] = jnp.zeros_like(out_ref)

    def one_block(b, carry):
        here = pl.ds(pl.multiple_of(b * rows, rows), rows)
        x, y, z = points_ref[0, here], points_ref[1, here], points_ref[2, here]
        square = 1.0 + 2.0 * (x * x + y * y + z * z)
        for row, value in enumerate((x, y, z, jnp.ones_like(x), square)):
            for half in range(x.shape[1] // 128):
                lanes = slice(half * 128, half * 128 + 128)
                out_ref[half, pl.ds(b * rows * rows + row, rows, stride=rows), :] = value[:, lanes]
        return carry

    lax.fori_loop(0, segs // rows, one_block, 0, unroll=2)


def pieces(value):
    first = value.astype(jnp.bfloat16).astype(jnp.float32)
    rest = value - first
    second = rest.astype(jnp.bfloat16).astype(jnp.float32)
    return (first, second, rest - second)


def node_side(fetched_ref, start, step):
    raw = fetched_ref[pl.ds(start, 6, stride=step), :]
    raw = jnp.concatenate([raw, jnp.zeros((2, raw.shape[1]), jnp.float32)], axis=0)
    row = lax.broadcasted_iota(jnp.int32, raw.shape, 0)
    coord = jnp.where(row < 3, raw, 0.0)
    square = 2.0 * jnp.sum(coord * coord, axis=0, keepdims=True)
    extended = jnp.where(row == 3, square, jnp.where(row == 4, 1.0, -4.0 * coord))
    a, b, c = pieces(extended)
    stacked = jnp.concatenate([a, a, b, b, a, c], axis=0)
    disp = jnp.where(row < 3, 0.0, jnp.where(row == 6, 1.0, raw))
    high = disp.astype(jnp.bfloat16).astype(jnp.float32)
    lhs = jnp.concatenate([high, disp - high], axis=0)
    lhs = jnp.concatenate([lhs, lhs], axis=1).astype(jnp.bfloat16)
    return stacked.T.astype(jnp.bfloat16), lhs


def points_of(points_ref, s):
    here = pl.ds(pl.multiple_of(s * 8, 8), 8)
    return jnp.concatenate([points_ref[h, here] for h in range(points_ref.shape[0])], axis=1)


def point_side(points):
    a, b, c = pieces(points)
    return jnp.concatenate([a, b, a, b, c, a], axis=0).astype(jnp.bfloat16)


def kernel_values(node_op, point_op):
    dist = jnp.dot(node_op, point_op, preferred_element_type=jnp.float32)
    value = 1.0 / dist
    high = value.astype(jnp.bfloat16)
    low = (value - high.astype(jnp.float32)).astype(jnp.bfloat16)
    return jnp.concatenate([high, low], axis=0)


def stage_a(s, start, step, fetched_ref, points_ref, both_ref, lhs_ref, i):
    node_op, lhs = node_side(fetched_ref, start, step)
    lhs_ref[i] = lhs
    both_ref[i] = kernel_values(node_op, point_side(points_of(points_ref, s)))


def sums_of(both_ref, lhs_ref, i):
    sums = jnp.dot(lhs_ref[i], both_ref[i], preferred_element_type=jnp.float32)
    return sums[:8] + sums[8:]


def pri_kernel(capacity, plan_ref, fetched_ref, points_ref, out_ref, both_ref, lhs_ref):
    segs = plan_ref.shape[1]

    def first(s, i):
        stage_a(s, plan_ref[0, s], capacity, fetched_ref, points_ref, both_ref, lhs_ref, i)

    def second(s, i):
        sums = sums_of(both_ref, lhs_ref, i)
        out_ref[s] = sums * (1.0 / sums[6:7])

    for i in range(WIDE):
        first(i, i)

    def one_group(g, carry):
        base = g * (2 * WIDE)
        after = jnp.minimum(base + 2 * WIDE, segs - WIDE)
        for i in range(WIDE):
            second(base + i, i)
            first(base + WIDE + i, WIDE + i)
        for i in range(WIDE):
            second(base + WIDE + i, WIDE + i)
            first(after + i, i)
        return carry

    lax.fori_loop(0, segs // (2 * WIDE), one_group, 0)


def sec_kernel(early, capacity, *refs):
    plan_ref, count_ref, fetched_ref, points_ref, weights_ref = refs[:5]
    if early:
        far_ref, out_ref, both_ref, lhs_ref, left_ref, other_ref, sems = refs[5:]
        out_ref[...] = jnp.zeros_like(out_ref)
        low, high_end = 0, plan_ref[4, 0]
        copies = []
    else:
        far_ref, before_ref, out_ref, both_ref, lhs_ref, left_ref, other_ref, sems = refs[5:]
        low, high_end = plan_ref[4, 0], plan_ref.shape[1]
        copies = [pltpu.make_async_copy(before_ref, out_ref, sems.at[1])]
    copies.append(pltpu.make_async_copy(far_ref, other_ref, sems.at[0]))
    for copy in copies:
        copy.start()

    def entry(row, place):
        return plan_ref[row, jnp.minimum(low + place, high_end - 1)]

    def first(place, i):
        step = 1 if early else capacity - 1
        s, start = entry(1, place), entry(2, place)
        stage_a(s, start, step, fetched_ref, points_ref, both_ref, lhs_ref, i)

    def second(place, i):
        s = entry(1, place)
        sums = sums_of(both_ref, lhs_ref, i)
        inverse = 1.0 / sums[6:7]
        weights = weights_ref[pl.ds(s, 1), :]
        position = lax.broadcasted_iota(jnp.int32, weights.shape, 1)
        weights = jnp.where(position < count_ref[s], weights, 0.0)
        gap = (weights * inverse) * (sums * inverse - other_ref[s])
        high = gap.astype(jnp.bfloat16).astype(jnp.float32)
        left_ref[i] = jnp.concatenate([high, gap - high], axis=0).astype(jnp.bfloat16)

    def third(place, i):
        left, both = left_ref[i], both_ref[i]
        half = both.shape[0] // 2
        if i % 2 == 0:
            result = lax.dot_general(
                left, both, (((1,), (1,)), ((), ())), preferred_element_type=jnp.float32
            )
            result = result[:8] + result[8:]
            result = result[:, :half] + result[:, half:]
        else:
            result = lax.dot_general(
                both, left, (((1,), (1,)), ((), ())), preferred_element_type=jnp.float32
            )
            result = (result[:half] + result[half:]).T
            result = result[:8] + result[8:]
        out_ref[pl.ds(entry(3, place), 3, stride=capacity), :] = result[3:6]

    for i in range(HALF):
        first(i, i)
    for copy in copies:
        copy.wait()

    def one_group(g, carry):
        base = g * (2 * HALF)
        for i in range(HALF):
            second(base + i, i)
            first(base + HALF + i, HALF + i)
        for i in range(HALF):
            third(base + i, i)
            second(base + HALF + i, HALF + i)
        for i in range(HALF):
            third(base + HALF + i, HALF + i)
            first(base + 2 * HALF + i, i)
        return carry

    lax.fori_loop(0, (high_end - low + 2 * HALF - 1) // (2 * HALF), one_group, 0)


def body(node_coords, node_disp, qpoints, qweights, qcount, sec_block, pri_block):
    devices = lax.axis_size("gx") * lax.axis_size("gy")
    blocks = node_coords.shape[0]
    nodes = node_coords.shape[2]
    segs = qpoints.shape[0]
    quad = qpoints.shape[2]
    slots = 2 * segs
    cap = slots // devices
    f32 = jnp.float32
    smem = pl.BlockSpec(memory_space=pltpu.SMEM)
    vmem = pl.BlockSpec(memory_space=pltpu.VMEM)

    limit = pltpu.CompilerParams(vmem_limit_bytes=16 * 1024 * 1024)

    def near(value):
        return pltpu.with_memory_space_constraint(value, pltpu.VMEM)

    def far(value):
        return pltpu.with_memory_space_constraint(value, pltpu.HBM)

    def exchange(value):
        return lax.all_to_all(value, AXES, split_axis=0, concat_axis=0, tiled=True)

    plan, request = pl.pallas_call(
        functools.partial(plan_kernel, devices, cap, blocks),
        out_shape=(
            jax.ShapeDtypeStruct((8, segs), jnp.int32),
            jax.ShapeDtypeStruct((devices, 128), f32),
        ),
        in_specs=[vmem, vmem],
        out_specs=(vmem, vmem),
        compiler_params=limit,
    )(sec_block.reshape(1, segs), pri_block.reshape(1, segs))
    xc = jnp.transpose(node_coords, (1, 0, 2)).reshape(3 * blocks, nodes)
    xu = jnp.transpose(node_disp, (1, 0, 2)).reshape(3 * blocks, nodes)
    hbm = pl.BlockSpec(memory_space=pltpu.HBM)
    table = pl.pallas_call(
        table_kernel,
        out_shape=pltpu.VMEM((8 * blocks, nodes), f32),
        in_specs=[vmem, vmem],
        out_specs=vmem,
        compiler_params=limit,
    )(far(xc), far(xu))
    received = exchange(request.reshape(devices, 1, 128)).reshape(devices, 128)
    sec_ids = received[:, :cap].reshape(slots).astype(jnp.int32)

    def scratch(count):
        return [
            pltpu.VMEM((2 * count, 2 * nodes, quad), jnp.bfloat16),
            pltpu.VMEM((2 * count, 16, 2 * nodes), jnp.bfloat16),
        ]

    def gather(first, rows):
        return pl.pallas_call(
            functools.partial(gather_kernel, devices, cap, first),
            out_shape=pltpu.HBM((devices * rows, nodes), f32),
            in_specs=[vmem, vmem],
            out_specs=vmem,
            scratch_shapes=[
                pltpu.VMEM((2 * cap, devices), jnp.int32),
                pltpu.SMEM((2 * cap, devices), jnp.int32),
                pltpu.SemaphoreType.DMA,
            ],
            compiler_params=limit,
        )(received, near(table)).reshape(devices, rows // 2, 2, nodes)

    out1 = gather(True, 6 * cap + 6)
    out2 = gather(False, 6 * cap - 6)
    in1 = near(exchange(out1).reshape(-1, nodes))
    in2 = near(exchange(out2).reshape(-1, nodes))
    points = pl.pallas_call(
        pack_kernel,
        out_shape=pltpu.VMEM((quad // 128, segs * 8, 128), f32),
        in_specs=[vmem],
        out_specs=vmem,
        compiler_params=limit,
    )(jnp.transpose(qpoints, (1, 0, 2)))
    points = near(points)
    other = pl.pallas_call(
        functools.partial(pri_kernel, cap),
        out_shape=pltpu.HBM((segs, 8, quad), f32),
        in_specs=[smem, vmem, vmem],
        out_specs=vmem,
        compiler_params=limit,
        scratch_shapes=scratch(WIDE),
    )(plan, in1, points)

    def secondary(early_part, *args):
        return pl.pallas_call(
            functools.partial(sec_kernel, early_part, cap),
            out_shape=pltpu.HBM((devices * 3 * cap, nodes), f32),
            in_specs=[smem] * 2 + [vmem] * 3 + [hbm] * (len(args) - 5),
            out_specs=vmem,
            compiler_params=limit,
            scratch_shapes=scratch(HALF)
            + [
                pltpu.VMEM((2 * HALF, 16, quad), jnp.bfloat16),
                pltpu.VMEM((segs, 8, quad), f32),
                pltpu.SemaphoreType.DMA((2,)),
            ],
        )(*args)

    other = far(other)
    parcels = secondary(True, plan, qcount, in1, points, qweights, other)
    parcels = far(parcels)
    parcels = secondary(False, plan, qcount, in2, points, qweights, other, parcels)
    incoming = exchange(parcels.reshape(devices, 3, cap, nodes))
    select = (jnp.arange(blocks, dtype=jnp.int32)[:, None] == sec_ids[None, :]).astype(f32)
    incoming = jnp.transpose(incoming, (0, 2, 1, 3)).reshape(slots, 3, nodes)
    return jnp.einsum("bp,pcn->bcn", select, incoming, precision=lax.Precision.HIGHEST)


def solution(mesh):
    split3 = P(AXES, None, None)
    placed = (split3, split3, split3, P(AXES, None), P(AXES), P(AXES), P(AXES))
    return jax.shard_map(body, mesh=mesh, in_specs=placed, out_specs=split3, check_vma=False)
```

```python
import functools
import jax
import jax.numpy as jnp
from jax import lax
from jax.experimental import pallas as pl
from jax.experimental.pallas import tpu as pltpu
from jax.sharding import PartitionSpec as P

AXES = ("gx", "gy")
WIDE = 16
SETS = 8


def strict_upper(size):
    row = lax.broadcasted_iota(jnp.int32, (size, size), 0)
    column = lax.broadcasted_iota(jnp.int32, (size, size), 1)
    return jnp.where(row < column, 1.0, 0.0).astype(jnp.bfloat16)


def dot_last(left, right):
    return lax.dot_general(
        left, right, (((1,), (1,)), ((), ())), preferred_element_type=jnp.float32
    )


def plan_kernel(devices, capacity, blocks, sec_ref, pri_ref, plan_ref, request_ref):
    segs = sec_ref.shape[1]
    upper = strict_upper(segs)
    device = lax.broadcasted_iota(jnp.int32, (devices, segs), 0).astype(jnp.float32)
    column = lax.broadcasted_iota(jnp.int32, (request_ref.shape[1], segs), 0).astype(jnp.float32)
    request = jnp.zeros(request_ref.shape, jnp.float32)
    routes = []
    for side, ref in enumerate((sec_ref, pri_ref)):
        ids = ref[...].astype(jnp.float32)
        owner = jnp.floor((ids + 0.5) * (1.0 / blocks))
        local = ids - owner * blocks
        mine = jnp.where(device == owner, 1.0, 0.0)
        narrow = mine.astype(jnp.bfloat16)
        before = jnp.dot(narrow, upper, preferred_element_type=jnp.float32)
        rank = jnp.sum(mine * before, axis=0, keepdims=True)
        coarse = jnp.floor(local * (1.0 / 16.0)) * 16.0
        here = column == rank + side * capacity
        for part in (coarse, local - coarse):
            request += dot_last(narrow, jnp.where(here, part, 0.0).astype(jnp.bfloat16))
        routes.append((owner, rank))
    request_ref[...] = request

    (sec_owner, sec_rank), (pri_owner, pri_rank) = routes
    early = jnp.where(sec_rank == 0.0, 1.0, 0.0)
    spread = jnp.broadcast_to(early, (16, segs)).astype(jnp.bfloat16)
    ahead = jnp.dot(spread, upper, preferred_element_type=jnp.float32)[:1]
    count = jnp.sum(early, axis=1, keepdims=True)
    number = lax.broadcasted_iota(jnp.int32, (1, segs), 1).astype(jnp.float32)
    place = jnp.where(sec_rank == 0.0, ahead, count + number - ahead)
    target = lax.broadcasted_iota(jnp.int32, (segs, segs), 0).astype(jnp.float32)
    moved = jnp.where(target == place, 1.0, 0.0).astype(jnp.bfloat16)
    row = lax.broadcasted_iota(jnp.int32, (16, segs), 0)
    values = jnp.where(row == 0, number, jnp.where(row == 1, sec_owner, sec_rank))
    values = dot_last(values.astype(jnp.bfloat16), moved)
    seg, dev, rank = values[0:1], values[1:2], values[2:3]
    start = jnp.where(
        rank == 0.0,
        dev * (6 * capacity + 6) + 6 * capacity,
        dev * (6 * capacity - 6) + (rank - 1.0),
    )
    rows = (
        pri_owner * (6 * capacity + 6) + pri_rank,
        seg,
        start,
        dev * (3 * capacity) + rank,
        jnp.broadcast_to(count, (1, segs)),
    )
    plan_ref[...] = jnp.zeros_like(plan_ref)
    for i, value in enumerate(rows):
        plan_ref[i : i + 1, :] = value.astype(jnp.int32)


def table_kernel(xc_ref, xu_ref, out_ref):
    blocks = xc_ref.shape[0] // 3

    def one_block(b, carry):
        for half, ref in enumerate((xc_ref, xu_ref)):
            for c in range(3):
                here = pl.ds(pl.multiple_of(c * blocks + b * 8, 8), 8)
                out_ref[pl.ds(b * 64 + 3 * half + c, 8, stride=8), :] = ref[here, :]
        return carry

    lax.fori_loop(0, blocks // 8, one_block, 0, unroll=4)


def gather_kernel(devices, capacity, first, ids_ref, table_ref, out_ref, turned, local_ref, sem):
    turned[...] = ids_ref[...].T[: 2 * capacity].astype(jnp.int32)
    copy = pltpu.make_async_copy(turned, local_ref, sem)
    copy.start()
    copy.wait()
    if first:
        parts = [(1, rank, rank, capacity) for rank in range(capacity)]
        parts.append((0, 0, 6 * capacity, 1))
    else:
        parts = [(0, rank, rank - 1, capacity - 1) for rank in range(1, capacity)]
    rows = 6 * len(parts)

    def one_device(dev, carry):
        for side, rank, start, step in parts:
            local = local_ref[side * capacity + rank, dev]
            patch = table_ref[pl.ds(pl.multiple_of(local * 8, 8), 8), :]
            out_ref[pl.ds(dev * rows + start, 6, stride=step), :] = patch[:6]
        return carry

    lax.fori_loop(0, devices, one_device, 0, unroll=4)


def pack_kernel(points_ref, out_ref):
    rows = 8
    segs = points_ref.shape[1]
    out_ref[...] = jnp.zeros_like(out_ref)

    def one_block(b, carry):
        here = pl.ds(pl.multiple_of(b * rows, rows), rows)
        x, y, z = points_ref[0, here], points_ref[1, here], points_ref[2, here]
        square = 1.0 + 2.0 * (x * x + y * y + z * z)
        for row, value in enumerate((x, y, z, jnp.ones_like(x), square)):
            for half in range(x.shape[1] // 128):
                lanes = slice(half * 128, half * 128 + 128)
                out_ref[half, pl.ds(b * rows * rows + row, rows, stride=rows), :] = value[:, lanes]
        return carry

    lax.fori_loop(0, segs // rows, one_block, 0, unroll=2)


def pieces(value):
    first = value.astype(jnp.bfloat16).astype(jnp.float32)
    rest = value - first
    second = rest.astype(jnp.bfloat16).astype(jnp.float32)
    return (first, second, rest - second)


def node_side(fetched_ref, start, step):
    raw = fetched_ref[pl.ds(start, 6, stride=step), :]
    raw = jnp.concatenate([raw, jnp.zeros((2, raw.shape[1]), jnp.float32)], axis=0)
    row = lax.broadcasted_iota(jnp.int32, raw.shape, 0)
    coord = jnp.where(row < 3, raw, 0.0)
    square = 2.0 * jnp.sum(coord * coord, axis=0, keepdims=True)
    extended = jnp.where(row == 3, square, jnp.where(row == 4, 1.0, -4.0 * coord))
    a, b, c = pieces(extended)
    stacked = jnp.concatenate([a, a, b, b, a, c], axis=0)
    disp = jnp.where(row < 3, 0.0, jnp.where(row == 6, 1.0, raw))
    high = disp.astype(jnp.bfloat16).astype(jnp.float32)
    lhs = jnp.concatenate([high, disp - high], axis=0)
    lhs = jnp.concatenate([lhs, lhs], axis=1).astype(jnp.bfloat16)
    return stacked.T.astype(jnp.bfloat16), lhs


def points_of(points_ref, s):
    here = pl.ds(pl.multiple_of(s * 8, 8), 8)
    return jnp.concatenate([points_ref[h, here] for h in range(points_ref.shape[0])], axis=1)


def point_side(points):
    a, b, c = pieces(points)
    return jnp.concatenate([a, b, a, b, c, a], axis=0).astype(jnp.bfloat16)


def kernel_values(node_op, point_op):
    dist = jnp.dot(node_op, point_op, preferred_element_type=jnp.float32)
    value = 1.0 / dist
    high = value.astype(jnp.bfloat16)
    low = (value - high.astype(jnp.float32)).astype(jnp.bfloat16)
    return jnp.concatenate([high, low], axis=0)


def stage_a(s, start, step, fetched_ref, points_ref, both_ref, lhs_ref, i):
    node_op, lhs = node_side(fetched_ref, start, step)
    lhs_ref[i] = lhs
    both_ref[i] = kernel_values(node_op, point_side(points_of(points_ref, s)))


def sums_of(both_ref, lhs_ref, i):
    sums = jnp.dot(lhs_ref[i], both_ref[i], preferred_element_type=jnp.float32)
    return sums[:8] + sums[8:]


def primary_pass(capacity, plan_ref, fetched_ref, points_ref, other_ref, both_ref, lhs_ref):
    segs = plan_ref.shape[1]

    def first(s, i):
        stage_a(s, plan_ref[0, s], capacity, fetched_ref, points_ref, both_ref, lhs_ref, i)

    def second(s, i):
        sums = sums_of(both_ref, lhs_ref, i)
        other_ref[s] = sums * (1.0 / sums[6:7])

    for i in range(WIDE):
        first(i, i)

    def one_group(g, carry):
        base = g * (2 * WIDE)
        after = jnp.minimum(base + 2 * WIDE, segs - WIDE)
        for i in range(WIDE):
            second(base + i, i)
            first(base + WIDE + i, WIDE + i)
        for i in range(WIDE):
            second(base + WIDE + i, WIDE + i)
            first(after + i, i)
        return carry

    lax.fori_loop(0, segs // (2 * WIDE), one_group, 0)


def secondary_pass(step, capacity, low, end, wait, refs):
    plan_ref, count_ref, fetched_ref, points_ref, weights_ref, other_ref = refs[:6]
    out_ref, both_ref, lhs_ref, left_ref = refs[6:]

    def entry(row, place):
        return plan_ref[row, jnp.minimum(low + place, end - 1)]

    def first(place, i):
        s, start = entry(1, place), entry(2, place)
        stage_a(s, start, step, fetched_ref, points_ref, both_ref, lhs_ref, i)

    def second(place, i):
        s = entry(1, place)
        sums = sums_of(both_ref, lhs_ref, i)
        inverse = 1.0 / sums[6:7]
        weights = weights_ref[pl.ds(s, 1), :]
        position = lax.broadcasted_iota(jnp.int32, weights.shape, 1)
        weights = jnp.where(position < count_ref[s], weights, 0.0)
        gap = (weights * inverse) * (sums * inverse - other_ref[s])
        high = gap.astype(jnp.bfloat16).astype(jnp.float32)
        left_ref[i] = jnp.concatenate([high, gap - high], axis=0).astype(jnp.bfloat16)

    def third(place, i):
        left, both = left_ref[i], both_ref[i]
        half = both.shape[0] // 2
        if i % 2 == 0:
            result = dot_last(left, both)
            result = result[:8] + result[8:]
            result = result[:, :half] + result[:, half:]
        else:
            result = dot_last(both, left)
            result = (result[:half] + result[half:]).T
            result = result[:8] + result[8:]
        out_ref[pl.ds(entry(3, place), 3, stride=capacity), :] = result[3:6]

    for i in range(SETS):
        first(i, i)
    wait()
    for i in range(SETS):
        second(i, i)
        first(SETS + i, SETS + i)

    def one_group(g, carry):
        base = g * (3 * SETS)
        for phase in range(3):
            for i in range(SETS):
                a, b, c = (phase * SETS + SETS * t + i for t in (2, 1, 0))
                third(base + c, c)
                second(base + b, b % (3 * SETS))
                first(base + a, a % (3 * SETS))
        return carry

    lax.fori_loop(0, (end - low + 3 * SETS - 1) // (3 * SETS), one_group, 0)


def early_kernel(capacity, plan_ref, count_ref, fetched_ref, points_ref, far_weights_ref, *refs):
    far_other_ref, out_ref, both_ref, lhs_ref, left_ref, other_ref, weights_ref, sems = refs
    load = pltpu.make_async_copy(far_weights_ref, weights_ref, sems.at[0])
    store = pltpu.make_async_copy(other_ref, far_other_ref, sems.at[1])
    load.start()
    out_ref[...] = jnp.zeros_like(out_ref)
    primary_pass(capacity, plan_ref, fetched_ref, points_ref, other_ref, both_ref, lhs_ref)
    store.start()
    secondary_pass(
        1,
        capacity,
        0,
        plan_ref[4, 0],
        load.wait,
        (plan_ref, count_ref, fetched_ref, points_ref, weights_ref, other_ref)
        + (out_ref, both_ref, lhs_ref, left_ref),
    )
    store.wait()


def late_kernel(capacity, plan_ref, count_ref, fetched_ref, points_ref, *refs):
    far_weights_ref, far_other_ref, before_ref, out_ref = refs[:4]
    both_ref, lhs_ref, left_ref, other_ref, weights_ref, sems = refs[4:]
    loads = [
        pltpu.make_async_copy(far_other_ref, other_ref, sems.at[0]),
        pltpu.make_async_copy(far_weights_ref, weights_ref, sems.at[1]),
        pltpu.make_async_copy(before_ref, out_ref, sems.at[2]),
    ]
    for load in loads:
        load.start()

    def wait():
        for load in loads:
            load.wait()

    secondary_pass(
        capacity - 1,
        capacity,
        plan_ref[4, 0],
        plan_ref.shape[1],
        wait,
        (plan_ref, count_ref, fetched_ref, points_ref, weights_ref, other_ref)
        + (out_ref, both_ref, lhs_ref, left_ref),
    )


def body(node_coords, node_disp, qpoints, qweights, qcount, sec_block, pri_block):
    devices = lax.axis_size("gx") * lax.axis_size("gy")
    blocks = node_coords.shape[0]
    nodes = node_coords.shape[2]
    segs = qpoints.shape[0]
    quad = qpoints.shape[2]
    slots = 2 * segs
    cap = slots // devices
    f32 = jnp.float32
    smem = pl.BlockSpec(memory_space=pltpu.SMEM)
    vmem = pl.BlockSpec(memory_space=pltpu.VMEM)

    limit = pltpu.CompilerParams(vmem_limit_bytes=16 * 1024 * 1024)

    def near(value):
        return pltpu.with_memory_space_constraint(value, pltpu.VMEM)

    def far(value):
        return pltpu.with_memory_space_constraint(value, pltpu.HBM)

    def exchange(value):
        return lax.all_to_all(value, AXES, split_axis=0, concat_axis=0, tiled=True)

    plan, request = pl.pallas_call(
        functools.partial(plan_kernel, devices, cap, blocks),
        out_shape=(
            jax.ShapeDtypeStruct((8, segs), jnp.int32),
            jax.ShapeDtypeStruct((devices, 128), f32),
        ),
        in_specs=[vmem, vmem],
        out_specs=(vmem, vmem),
        compiler_params=limit,
    )(far(sec_block.reshape(1, segs)), far(pri_block.reshape(1, segs)))
    xc = jnp.transpose(node_coords, (1, 0, 2)).reshape(3 * blocks, nodes)
    xu = jnp.transpose(node_disp, (1, 0, 2)).reshape(3 * blocks, nodes)
    hbm = pl.BlockSpec(memory_space=pltpu.HBM)
    table = pl.pallas_call(
        table_kernel,
        out_shape=pltpu.VMEM((8 * blocks, nodes), f32),
        in_specs=[vmem, vmem],
        out_specs=vmem,
        compiler_params=limit,
    )(far(xc), far(xu))
    received = exchange(request.reshape(devices, 1, 128)).reshape(devices, 128)
    sec_ids = received[:, :cap].reshape(slots).astype(jnp.int32)

    def gather(first, rows):
        return pl.pallas_call(
            functools.partial(gather_kernel, devices, cap, first),
            out_shape=pltpu.HBM((devices * rows, nodes), f32),
            in_specs=[vmem, vmem],
            out_specs=vmem,
            scratch_shapes=[
                pltpu.VMEM((2 * cap, devices), jnp.int32),
                pltpu.SMEM((2 * cap, devices), jnp.int32),
                pltpu.SemaphoreType.DMA,
            ],
            compiler_params=limit,
        )(received, near(table)).reshape(devices, rows // 2, 2, nodes)

    out1 = gather(True, 6 * cap + 6)
    out2 = gather(False, 6 * cap - 6)
    in1 = near(exchange(out1).reshape(-1, nodes))
    in2 = near(exchange(out2).reshape(-1, nodes))
    points = pl.pallas_call(
        pack_kernel,
        out_shape=pltpu.VMEM((quad // 128, segs * 8, 128), f32),
        in_specs=[vmem],
        out_specs=vmem,
        compiler_params=limit,
    )(jnp.transpose(qpoints, (1, 0, 2)))
    points = near(points)

    def scratch(count, sems):
        return [
            pltpu.VMEM((count, 2 * nodes, quad), jnp.bfloat16),
            pltpu.VMEM((count, 16, 2 * nodes), jnp.bfloat16),
            pltpu.VMEM((3 * SETS, 16, quad), jnp.bfloat16),
            pltpu.VMEM((segs, 8, quad), f32),
            pltpu.VMEM((segs, quad), f32),
            pltpu.SemaphoreType.DMA((sems,)),
        ]

    parcel = pltpu.HBM((devices * 3 * cap, nodes), f32)
    weights = far(qweights)
    other, parcels = pl.pallas_call(
        functools.partial(early_kernel, cap),
        out_shape=(pltpu.HBM((segs, 8, quad), f32), parcel),
        in_specs=[smem, smem, vmem, vmem, hbm],
        out_specs=(hbm, vmem),
        scratch_shapes=scratch(max(2 * WIDE, 3 * SETS), 2),
        compiler_params=limit,
    )(plan, qcount, in1, points, weights)
    parcels = pl.pallas_call(
        functools.partial(late_kernel, cap),
        out_shape=parcel,
        in_specs=[smem, smem, vmem, vmem, hbm, hbm, hbm],
        out_specs=vmem,
        scratch_shapes=scratch(3 * SETS, 3),
        compiler_params=limit,
    )(plan, qcount, in2, points, weights, far(other), far(parcels))
    incoming = exchange(parcels.reshape(devices, 3, cap, nodes))
    select = (jnp.arange(blocks, dtype=jnp.int32)[:, None] == sec_ids[None, :]).astype(f32)
    incoming = jnp.transpose(incoming, (0, 2, 1, 3)).reshape(slots, 3, nodes)
    return jnp.einsum("bp,pcn->bcn", select, incoming, precision=lax.Precision.HIGHEST)


def solution(mesh):
    split3 = P(AXES, None, None)
    placed = (split3, split3, split3, P(AXES, None), P(AXES), P(AXES), P(AXES))
    return jax.shard_map(body, mesh=mesh, in_specs=placed, out_specs=split3, check_vma=False)
```

```python
import functools
import jax
import jax.numpy as jnp
from jax import lax
from jax.experimental import pallas as pl
from jax.experimental.pallas import tpu as pltpu
from jax.sharding import PartitionSpec as P

AXES = ("gx", "gy")
WIDE = 16
SETS = 8
CHUNKS = 4


def strict_upper(size):
    row = lax.broadcasted_iota(jnp.int32, (size, size), 0)
    column = lax.broadcasted_iota(jnp.int32, (size, size), 1)
    return jnp.where(row < column, 1.0, 0.0).astype(jnp.bfloat16)


def dot_last(left, right):
    return lax.dot_general(
        left, right, (((1,), (1,)), ((), ())), preferred_element_type=jnp.float32
    )


def plan_kernel(devices, capacity, blocks, sec_ref, pri_ref, plan_ref, request_ref):
    segs = sec_ref.shape[1]
    upper = strict_upper(segs)
    device = lax.broadcasted_iota(jnp.int32, (devices, segs), 0).astype(jnp.float32)
    column = lax.broadcasted_iota(jnp.int32, (request_ref.shape[1], segs), 0).astype(jnp.float32)
    request = jnp.zeros(request_ref.shape, jnp.float32)
    routes = []
    for side, ref in enumerate((sec_ref, pri_ref)):
        ids = ref[...].astype(jnp.float32)
        owner = jnp.floor((ids + 0.5) * (1.0 / blocks))
        local = ids - owner * blocks
        mine = jnp.where(device == owner, 1.0, 0.0)
        narrow = mine.astype(jnp.bfloat16)
        before = jnp.dot(narrow, upper, preferred_element_type=jnp.float32)
        rank = jnp.sum(mine * before, axis=0, keepdims=True)
        coarse = jnp.floor(local * (1.0 / 16.0)) * 16.0
        here = column == rank + side * capacity
        for part in (coarse, local - coarse):
            request += dot_last(narrow, jnp.where(here, part, 0.0).astype(jnp.bfloat16))
        routes.append((owner, rank))
    request_ref[...] = request

    (sec_owner, sec_rank), (pri_owner, pri_rank) = routes
    early = jnp.where(sec_rank == 0.0, 1.0, 0.0)
    spread = jnp.broadcast_to(early, (16, segs)).astype(jnp.bfloat16)
    ahead = jnp.dot(spread, upper, preferred_element_type=jnp.float32)[:1]
    count = jnp.sum(early, axis=1, keepdims=True)
    number = lax.broadcasted_iota(jnp.int32, (1, segs), 1).astype(jnp.float32)
    place = jnp.where(sec_rank == 0.0, ahead, count + number - ahead)
    target = lax.broadcasted_iota(jnp.int32, (segs, segs), 0).astype(jnp.float32)
    moved = jnp.where(target == place, 1.0, 0.0).astype(jnp.bfloat16)
    row = lax.broadcasted_iota(jnp.int32, (16, segs), 0)
    values = jnp.where(row == 0, number, jnp.where(row == 1, sec_owner, sec_rank))
    values = dot_last(values.astype(jnp.bfloat16), moved)
    seg, dev, rank = values[0:1], values[1:2], values[2:3]
    start = jnp.where(
        rank == 0.0,
        dev * (6 * capacity + 6) + 6 * capacity,
        dev * (6 * capacity - 6) + (rank - 1.0),
    )
    rows = (
        pri_owner * (6 * capacity + 6) + pri_rank,
        seg,
        start,
        dev * (3 * capacity) + rank,
        jnp.broadcast_to(count, (1, segs)),
        dev * 3.0,
    )
    plan_ref[...] = jnp.zeros_like(plan_ref)
    for i, value in enumerate(rows):
        plan_ref[i : i + 1, :] = value.astype(jnp.int32)


def table_kernel(xc_ref, xu_ref, out_ref):
    blocks = xc_ref.shape[0] // 3

    def one_block(b, carry):
        for half, ref in enumerate((xc_ref, xu_ref)):
            for c in range(3):
                here = pl.ds(pl.multiple_of(c * blocks + b * 8, 8), 8)
                out_ref[pl.ds(b * 64 + 3 * half + c, 8, stride=8), :] = ref[here, :]
        return carry

    lax.fori_loop(0, blocks // 8, one_block, 0, unroll=4)


def gather_kernel(devices, capacity, first, ids_ref, table_ref, *refs):
    far_ref, turned_ref, near_ref, local_ref, sem, sems = refs
    turned_ref[...] = ids_ref[...].T[: 2 * capacity].astype(jnp.int32)
    copy = pltpu.make_async_copy(turned_ref, local_ref, sem)
    copy.start()
    copy.wait()
    if first:
        parts = [(1, rank, rank, capacity) for rank in range(capacity)]
        parts.append((0, 0, 6 * capacity, 1))
    else:
        parts = [(0, rank, rank - 1, capacity - 1) for rank in range(1, capacity)]
    rows = 6 * len(parts)

    def one_device(dev, carry):
        for side, rank, start, step in parts:
            local = local_ref[side * capacity + rank, dev]
            patch = table_ref[pl.ds(pl.multiple_of(local * 8, 8), 8), :]
            near_ref[pl.ds(dev * rows + start, 6, stride=step), :] = patch[:6]
        return carry

    part = devices // CHUNKS
    stores = []
    for chunk in range(CHUNKS):
        lax.fori_loop(chunk * part, (chunk + 1) * part, one_device, 0, unroll=4)
        here = pl.ds(chunk * part * rows, part * rows)
        stores.append(pltpu.make_async_copy(near_ref.at[here], far_ref.at[here], sems.at[chunk]))
        stores[-1].start()
    for store in stores:
        store.wait()


def pack_kernel(points_ref, out_ref):
    rows = 8
    segs = points_ref.shape[1]
    out_ref[...] = jnp.zeros_like(out_ref)

    def one_block(b, carry):
        here = pl.ds(pl.multiple_of(b * rows, rows), rows)
        x, y, z = points_ref[0, here], points_ref[1, here], points_ref[2, here]
        square = 1.0 + 2.0 * (x * x + y * y + z * z)
        for row, value in enumerate((x, y, z, jnp.ones_like(x), square)):
            for half in range(x.shape[1] // 128):
                lanes = slice(half * 128, half * 128 + 128)
                out_ref[half, pl.ds(b * rows * rows + row, rows, stride=rows), :] = value[:, lanes]
        return carry

    lax.fori_loop(0, segs // rows, one_block, 0, unroll=2)


def pieces(value):
    first = value.astype(jnp.bfloat16).astype(jnp.float32)
    rest = value - first
    second = rest.astype(jnp.bfloat16).astype(jnp.float32)
    return (first, second, rest - second)


def node_side(fetched_ref, start, step):
    raw = fetched_ref[pl.ds(start, 6, stride=step), :]
    raw = jnp.concatenate([raw, jnp.zeros((2, raw.shape[1]), jnp.float32)], axis=0)
    row = lax.broadcasted_iota(jnp.int32, raw.shape, 0)
    coord = jnp.where(row < 3, raw, 0.0)
    square = 2.0 * jnp.sum(coord * coord, axis=0, keepdims=True)
    extended = jnp.where(row == 3, square, jnp.where(row == 4, 1.0, -4.0 * coord))
    a, b, c = pieces(extended)
    stacked = jnp.concatenate([a, a, b, b, a, c], axis=0)
    disp = jnp.where(row < 3, 0.0, jnp.where(row == 6, 1.0, raw))
    high = disp.astype(jnp.bfloat16).astype(jnp.float32)
    lhs = jnp.concatenate([high, disp - high], axis=0)
    lhs = jnp.concatenate([lhs, lhs], axis=1).astype(jnp.bfloat16)
    return stacked.astype(jnp.bfloat16).T, lhs


def points_of(points_ref, s):
    here = pl.ds(pl.multiple_of(s * 8, 8), 8)
    return jnp.concatenate([points_ref[h, here] for h in range(points_ref.shape[0])], axis=1)


def point_side(points):
    a, b, c = pieces(points)
    return jnp.concatenate([a, b, a, b, c, a], axis=0).astype(jnp.bfloat16)


def kernel_values(node_op, point_op):
    dist = jnp.dot(node_op, point_op, preferred_element_type=jnp.float32)
    value = 1.0 / dist
    high = value.astype(jnp.bfloat16)
    low = (value - high.astype(jnp.float32)).astype(jnp.bfloat16)
    return jnp.concatenate([high, low], axis=0)


def stage_a(s, start, step, fetched_ref, points_ref, both_ref, lhs_ref, i):
    node_op, lhs = node_side(fetched_ref, start, step)
    lhs_ref[i] = lhs
    both_ref[i] = kernel_values(node_op, point_side(points_of(points_ref, s)))


def sums_of(both_ref, lhs_ref, i):
    sums = jnp.dot(lhs_ref[i], both_ref[i], preferred_element_type=jnp.float32)
    return sums[:8] + sums[8:]


def primary_pass(capacity, plan_ref, fetched_ref, points_ref, other_ref, both_ref, lhs_ref):
    segs = plan_ref.shape[1]

    def first(s, i):
        stage_a(s, plan_ref[0, s], capacity, fetched_ref, points_ref, both_ref, lhs_ref, i)

    def second(s, i):
        sums = sums_of(both_ref, lhs_ref, i)
        other_ref[s] = sums * (1.0 / sums[6:7])

    for i in range(WIDE):
        first(i, i)

    def one_group(g, carry):
        base = g * (2 * WIDE)
        after = jnp.minimum(base + 2 * WIDE, segs - WIDE)
        for i in range(WIDE):
            second(base + i, i)
            first(base + WIDE + i, WIDE + i)
        for i in range(WIDE):
            second(base + WIDE + i, WIDE + i)
            first(after + i, i)
        return carry

    lax.fori_loop(0, segs // (2 * WIDE), one_group, 0)


def secondary_pass(step, apart, base_row, low, end, wait, refs):
    plan_ref, count_ref, fetched_ref, points_ref, weights_ref, other_ref = refs[:6]
    out_ref, both_ref, lhs_ref, left_ref = refs[6:]

    def entry(row, place):
        return plan_ref[row, jnp.minimum(low + place, end - 1)]

    def first(place, i):
        s, start = entry(1, place), entry(2, place)
        stage_a(s, start, step, fetched_ref, points_ref, both_ref, lhs_ref, i)

    def second(place, i):
        s = entry(1, place)
        sums = sums_of(both_ref, lhs_ref, i)
        inverse = 1.0 / sums[6:7]
        weights = weights_ref[pl.ds(s, 1), :]
        position = lax.broadcasted_iota(jnp.int32, weights.shape, 1)
        weights = jnp.where(position < count_ref[s], weights, 0.0)
        gap = (weights * inverse) * (sums * inverse - other_ref[s])
        high = gap.astype(jnp.bfloat16).astype(jnp.float32)
        left_ref[i] = jnp.concatenate([high, gap - high], axis=0).astype(jnp.bfloat16)

    def third(place, i):
        left, both = left_ref[i], both_ref[i]
        half = both.shape[0] // 2
        if i % 2 == 0:
            result = dot_last(left, both)
            result = result[:8] + result[8:]
            result = result[:, :half] + result[:, half:]
        else:
            result = dot_last(both, left)
            result = (result[:half] + result[half:]).T
            result = result[:8] + result[8:]
        out_ref[pl.ds(entry(base_row, place), 3, stride=apart), :] = result[3:6]

    for i in range(2 * SETS):
        first(i, i)
    wait()
    for i in range(SETS):
        second(i, i)

    def one_group(g, carry):
        base = g * (3 * SETS)
        for phase in range(3):
            for i in range(SETS):
                a, b, c = (phase * SETS + SETS * t + i for t in (2, 1, 0))
                third(base + c, c)
                second(base + b, b % (3 * SETS))
                first(base + a, a % (3 * SETS))
        return carry

    lax.fori_loop(0, (end - low + 3 * SETS - 1) // (3 * SETS), one_group, 0)


def early_kernel(capacity, plan_ref, count_ref, fetched_ref, points_ref, far_weights_ref, *refs):
    far_other_ref, out_ref, both_ref, lhs_ref, left_ref, other_ref, weights_ref, sems = refs
    load = pltpu.make_async_copy(far_weights_ref, weights_ref, sems.at[0])
    store = pltpu.make_async_copy(other_ref, far_other_ref, sems.at[1])
    load.start()
    out_ref[...] = jnp.zeros_like(out_ref)
    primary_pass(capacity, plan_ref, fetched_ref, points_ref, other_ref, both_ref, lhs_ref)
    store.start()
    secondary_pass(
        1,
        1,
        5,
        0,
        plan_ref[4, 0],
        load.wait,
        (plan_ref, count_ref, fetched_ref, points_ref, weights_ref, other_ref)
        + (out_ref, both_ref, lhs_ref, left_ref),
    )
    store.wait()


def late_kernel(capacity, plan_ref, count_ref, fetched_ref, points_ref, *refs):
    far_weights_ref, far_other_ref, before_ref, out_ref = refs[:4]
    both_ref, lhs_ref, left_ref, other_ref, weights_ref, sems = refs[4:]
    loads = [
        pltpu.make_async_copy(far_other_ref, other_ref, sems.at[0]),
        pltpu.make_async_copy(far_weights_ref, weights_ref, sems.at[1]),
    ]
    for load in loads:
        load.start()
    out_ref[...] = jnp.zeros_like(out_ref)
    for row in range(0, before_ref.shape[0], 8):
        out_ref[pl.ds(row * capacity, 8, stride=capacity), :] = before_ref[row : row + 8, :]

    def wait():
        for load in loads:
            load.wait()

    secondary_pass(
        capacity - 1,
        capacity,
        3,
        plan_ref[4, 0],
        plan_ref.shape[1],
        wait,
        (plan_ref, count_ref, fetched_ref, points_ref, weights_ref, other_ref)
        + (out_ref, both_ref, lhs_ref, left_ref),
    )


def assemble_kernel(capacity, blocks, ids_ref, in_ref, out_ref):
    devices = ids_ref.shape[1]
    block = lax.broadcasted_iota(jnp.int32, (blocks, devices), 0)
    select, rows = [], []
    for rank in range(capacity):
        select.append(jnp.where(block == ids_ref[rank : rank + 1, :], 1.0, 0.0))
        step = 3 * capacity
        parts = [in_ref[pl.ds(c * capacity + rank, devices, stride=step), :] for c in range(3)]
        rows.append(jnp.concatenate(parts, axis=1))
    select = jnp.concatenate(select, axis=1).astype(jnp.bfloat16)
    total = None
    for piece in pieces(jnp.concatenate(rows, axis=0)):
        term = jnp.dot(select, piece.astype(jnp.bfloat16), preferred_element_type=jnp.float32)
        total = term if total is None else total + term
    nodes = in_ref.shape[1]
    for c in range(3):
        out_ref[c * blocks : (c + 1) * blocks, :] = total[:, c * nodes : (c + 1) * nodes]


def body(node_coords, node_disp, qpoints, qweights, qcount, sec_block, pri_block):
    devices = lax.axis_size("gx") * lax.axis_size("gy")
    blocks = node_coords.shape[0]
    nodes = node_coords.shape[2]
    segs = qpoints.shape[0]
    quad = qpoints.shape[2]
    slots = 2 * segs
    cap = slots // devices
    f32 = jnp.float32
    smem = pl.BlockSpec(memory_space=pltpu.SMEM)
    vmem = pl.BlockSpec(memory_space=pltpu.VMEM)

    limit = pltpu.CompilerParams(vmem_limit_bytes=16 * 1024 * 1024)

    def near(value):
        return pltpu.with_memory_space_constraint(value, pltpu.VMEM)

    def far(value):
        return pltpu.with_memory_space_constraint(value, pltpu.HBM)

    def exchange(value):
        return lax.all_to_all(value, AXES, split_axis=0, concat_axis=0, tiled=True)

    plan, request = pl.pallas_call(
        functools.partial(plan_kernel, devices, cap, blocks),
        out_shape=(
            jax.ShapeDtypeStruct((8, segs), jnp.int32),
            jax.ShapeDtypeStruct((devices, 128), f32),
        ),
        in_specs=[vmem, vmem],
        out_specs=(vmem, vmem),
        compiler_params=limit,
    )(far(sec_block.reshape(1, segs)), far(pri_block.reshape(1, segs)))
    xc = jnp.transpose(node_coords, (1, 0, 2)).reshape(3 * blocks, nodes)
    xu = jnp.transpose(node_disp, (1, 0, 2)).reshape(3 * blocks, nodes)
    hbm = pl.BlockSpec(memory_space=pltpu.HBM)
    table = pl.pallas_call(
        table_kernel,
        out_shape=pltpu.VMEM((8 * blocks, nodes), f32),
        in_specs=[vmem, vmem],
        out_specs=vmem,
        compiler_params=limit,
    )(far(xc), far(xu))
    received = exchange(request.reshape(devices, 1, 128)).reshape(devices, 128)

    def gather(first, rows):
        out, turned = pl.pallas_call(
            functools.partial(gather_kernel, devices, cap, first),
            out_shape=(
                pltpu.HBM((devices * rows, nodes), f32),
                jax.ShapeDtypeStruct((2 * cap, devices), jnp.int32),
            ),
            in_specs=[vmem, vmem],
            out_specs=(hbm, vmem),
            scratch_shapes=[
                pltpu.VMEM((devices * rows, nodes), f32),
                pltpu.SMEM((2 * cap, devices), jnp.int32),
                pltpu.SemaphoreType.DMA,
                pltpu.SemaphoreType.DMA((CHUNKS,)),
            ],
            compiler_params=limit,
        )(received, near(table))
        return out.reshape(devices, rows // 2, 2, nodes), turned

    out1, turned = gather(True, 6 * cap + 6)
    out2, _ = gather(False, 6 * cap - 6)
    in1 = near(exchange(out1).reshape(-1, nodes))
    in2 = near(exchange(out2).reshape(-1, nodes))
    points = pl.pallas_call(
        pack_kernel,
        out_shape=pltpu.VMEM((quad // 128, segs * 8, 128), f32),
        in_specs=[vmem],
        out_specs=vmem,
        compiler_params=limit,
    )(jnp.transpose(qpoints, (1, 0, 2)))
    points = near(points)

    def scratch(count, sems):
        return [
            pltpu.VMEM((count, 2 * nodes, quad), jnp.bfloat16),
            pltpu.VMEM((count, 16, 2 * nodes), jnp.bfloat16),
            pltpu.VMEM((3 * SETS, 16, quad), jnp.bfloat16),
            pltpu.VMEM((segs, 8, quad), f32),
            pltpu.VMEM((segs, quad), f32),
            pltpu.SemaphoreType.DMA((sems,)),
        ]

    weights = far(qweights)
    other, parcels = pl.pallas_call(
        functools.partial(early_kernel, cap),
        out_shape=(
            pltpu.HBM((segs, 8, quad), f32),
            jax.ShapeDtypeStruct((devices * 3, nodes), f32),
        ),
        in_specs=[smem, smem, vmem, vmem, hbm],
        out_specs=(hbm, vmem),
        scratch_shapes=scratch(max(2 * WIDE, 3 * SETS), 2),
        compiler_params=limit,
    )(plan, qcount, in1, points, weights)
    parcels = pl.pallas_call(
        functools.partial(late_kernel, cap),
        out_shape=pltpu.VMEM((devices * 3 * cap, nodes), f32),
        in_specs=[smem, smem, vmem, vmem, hbm, hbm, vmem],
        out_specs=vmem,
        scratch_shapes=scratch(3 * SETS, 2),
        compiler_params=limit,
    )(plan, qcount, in2, points, weights, far(other), parcels)
    incoming = exchange(parcels.reshape(devices, 3, cap, nodes)).reshape(-1, nodes)
    gap = pl.pallas_call(
        functools.partial(assemble_kernel, cap, blocks),
        out_shape=jax.ShapeDtypeStruct((3 * blocks, nodes), f32),
        in_specs=[vmem, vmem],
        out_specs=vmem,
        compiler_params=limit,
    )(turned, near(incoming))
    return jnp.transpose(gap.reshape(3, blocks, nodes), (1, 0, 2))


def solution(mesh):
    split3 = P(AXES, None, None)
    placed = (split3, split3, split3, P(AXES, None), P(AXES), P(AXES), P(AXES))
    return jax.shard_map(body, mesh=mesh, in_specs=placed, out_specs=split3, check_vma=False)
```

```python
import functools
import jax
import jax.numpy as jnp
from jax import lax
from jax.experimental import pallas as pl
from jax.experimental.pallas import tpu as pltpu
from jax.sharding import PartitionSpec as P

AXES = ("gx", "gy")
WIDE = 16
EARLY_SETS = 7
LATE_SETS = 8
CHUNKS = 4


def strict_upper(size):
    row = lax.broadcasted_iota(jnp.int32, (size, size), 0)
    column = lax.broadcasted_iota(jnp.int32, (size, size), 1)
    return jnp.where(row < column, 1.0, 0.0).astype(jnp.bfloat16)


def dot_last(left, right):
    return lax.dot_general(
        left, right, (((1,), (1,)), ((), ())), preferred_element_type=jnp.float32
    )


def plan_kernel(devices, capacity, blocks, sec_ref, pri_ref, plan_ref, request_ref):
    segs = sec_ref.shape[1]
    upper = strict_upper(segs)
    device = lax.broadcasted_iota(jnp.int32, (devices, segs), 0).astype(jnp.float32)
    column = lax.broadcasted_iota(jnp.int32, (request_ref.shape[1], segs), 0).astype(jnp.float32)
    request = jnp.zeros(request_ref.shape, jnp.float32)
    routes = []
    for side, ref in enumerate((sec_ref, pri_ref)):
        ids = ref[...].astype(jnp.float32)
        owner = jnp.floor((ids + 0.5) * (1.0 / blocks))
        local = ids - owner * blocks
        mine = jnp.where(device == owner, 1.0, 0.0)
        narrow = mine.astype(jnp.bfloat16)
        before = jnp.dot(narrow, upper, preferred_element_type=jnp.float32)
        rank = jnp.sum(mine * before, axis=0, keepdims=True)
        coarse = jnp.floor(local * (1.0 / 16.0)) * 16.0
        here = column == rank + side * capacity
        for part in (coarse, local - coarse):
            request += dot_last(narrow, jnp.where(here, part, 0.0).astype(jnp.bfloat16))
        routes.append((owner, rank))
    request_ref[...] = request

    (sec_owner, sec_rank), (pri_owner, pri_rank) = routes
    early = jnp.where(sec_rank == 0.0, 1.0, 0.0)
    spread = jnp.broadcast_to(early, (16, segs)).astype(jnp.bfloat16)
    ahead = jnp.dot(spread, upper, preferred_element_type=jnp.float32)[:1]
    count = jnp.sum(early, axis=1, keepdims=True)
    number = lax.broadcasted_iota(jnp.int32, (1, segs), 1).astype(jnp.float32)
    place = jnp.where(sec_rank == 0.0, ahead, count + number - ahead)
    target = lax.broadcasted_iota(jnp.int32, (segs, segs), 0).astype(jnp.float32)
    moved = jnp.where(target == place, 1.0, 0.0).astype(jnp.bfloat16)
    row = lax.broadcasted_iota(jnp.int32, (16, segs), 0)
    values = jnp.where(row == 0, number, jnp.where(row == 1, sec_owner, sec_rank))
    values = dot_last(values.astype(jnp.bfloat16), moved)
    seg, dev, rank = values[0:1], values[1:2], values[2:3]
    start = jnp.where(
        rank == 0.0,
        dev * (6 * capacity + 6) + 6 * capacity,
        dev * (6 * capacity - 6) + (rank - 1.0),
    )
    rows = (
        pri_owner * (6 * capacity + 6) + pri_rank,
        seg,
        start,
        dev * (3 * capacity) + rank,
        jnp.broadcast_to(count, (1, segs)),
        dev * 3.0,
    )
    plan_ref[...] = jnp.zeros_like(plan_ref)
    for i, value in enumerate(rows):
        plan_ref[i : i + 1, :] = value.astype(jnp.int32)


def table_kernel(xc_ref, xu_ref, out_ref):
    blocks = xc_ref.shape[0] // 3

    def one_block(b, carry):
        for half, ref in enumerate((xc_ref, xu_ref)):
            for c in range(3):
                here = pl.ds(pl.multiple_of(c * blocks + b * 8, 8), 8)
                out_ref[pl.ds(b * 64 + 3 * half + c, 8, stride=8), :] = ref[here, :]
        return carry

    lax.fori_loop(0, blocks // 8, one_block, 0, unroll=4)


def gather_kernel(devices, capacity, first, ids_ref, table_ref, *refs):
    far_ref, turned_ref, near_ref, local_ref, sem, sems = refs
    turned_ref[...] = ids_ref[...].T[: 2 * capacity].astype(jnp.int32)
    copy = pltpu.make_async_copy(turned_ref, local_ref, sem)
    copy.start()
    copy.wait()
    if first:
        parts = [(1, rank, rank, capacity) for rank in range(capacity)]
        parts.append((0, 0, 6 * capacity, 1))
    else:
        parts = [(0, rank, rank - 1, capacity - 1) for rank in range(1, capacity)]
    rows = 6 * len(parts)

    def one_device(dev, carry):
        for side, rank, start, step in parts:
            local = local_ref[side * capacity + rank, dev]
            patch = table_ref[pl.ds(pl.multiple_of(local * 8, 8), 8), :]
            near_ref[pl.ds(dev * rows + start, 6, stride=step), :] = patch[:6]
        return carry

    part = devices // CHUNKS
    stores = []
    for chunk in range(CHUNKS):
        lax.fori_loop(chunk * part, (chunk + 1) * part, one_device, 0, unroll=4)
        here = pl.ds(chunk * part * rows, part * rows)
        stores.append(pltpu.make_async_copy(near_ref.at[here], far_ref.at[here], sems.at[chunk]))
        stores[-1].start()
    for store in stores:
        store.wait()


def pack_kernel(points_ref, out_ref):
    rows = 8
    segs = points_ref.shape[1]
    out_ref[...] = jnp.zeros_like(out_ref)

    def one_block(b, carry):
        here = pl.ds(pl.multiple_of(b * rows, rows), rows)
        x, y, z = points_ref[0, here], points_ref[1, here], points_ref[2, here]
        square = 1.0 + 2.0 * (x * x + y * y + z * z)
        for row, value in enumerate((x, y, z, jnp.ones_like(x), square)):
            for half in range(x.shape[1] // 128):
                lanes = slice(half * 128, half * 128 + 128)
                out_ref[half, pl.ds(b * rows * rows + row, rows, stride=rows), :] = value[:, lanes]
        return carry

    lax.fori_loop(0, segs // rows, one_block, 0, unroll=2)


def pieces(value):
    first = value.astype(jnp.bfloat16).astype(jnp.float32)
    rest = value - first
    second = rest.astype(jnp.bfloat16).astype(jnp.float32)
    return (first, second, rest - second)


def node_side(fetched_ref, start, step):
    raw = fetched_ref[pl.ds(start, 6, stride=step), :]
    raw = jnp.concatenate([raw, jnp.zeros((2, raw.shape[1]), jnp.float32)], axis=0)
    row = lax.broadcasted_iota(jnp.int32, raw.shape, 0)
    coord = jnp.where(row < 3, raw, 0.0)
    square = 2.0 * jnp.sum(coord * coord, axis=0, keepdims=True)
    extended = jnp.where(row == 3, square, jnp.where(row == 4, 1.0, -4.0 * coord))
    a, b, c = pieces(extended)
    stacked = jnp.concatenate([a, a, b, b, a, c], axis=0)
    disp = jnp.where(row < 3, 0.0, jnp.where(row == 6, 1.0, raw))
    high = disp.astype(jnp.bfloat16).astype(jnp.float32)
    lhs = jnp.concatenate([high, disp - high], axis=0)
    lhs = jnp.concatenate([lhs, lhs], axis=1).astype(jnp.bfloat16)
    return stacked.astype(jnp.bfloat16).T, lhs


def points_of(points_ref, s):
    here = pl.ds(pl.multiple_of(s * 8, 8), 8)
    return jnp.concatenate([points_ref[h, here] for h in range(points_ref.shape[0])], axis=1)


def point_side(points):
    a, b, c = pieces(points)
    return jnp.concatenate([a, b, a, b, c, a], axis=0).astype(jnp.bfloat16)


def kernel_values(node_op, point_op):
    dist = jnp.dot(node_op, point_op, preferred_element_type=jnp.float32)
    value = 1.0 / dist
    high = value.astype(jnp.bfloat16)
    low = (value - high.astype(jnp.float32)).astype(jnp.bfloat16)
    return jnp.concatenate([high, low], axis=0)


def stage_a(s, start, step, fetched_ref, points_ref, both_ref, lhs_ref, i):
    node_op, lhs = node_side(fetched_ref, start, step)
    lhs_ref[i] = lhs
    both_ref[i] = kernel_values(node_op, point_side(points_of(points_ref, s)))


def sums_of(both_ref, lhs_ref, i):
    sums = jnp.dot(lhs_ref[i], both_ref[i], preferred_element_type=jnp.float32)
    return sums[:8] + sums[8:]


def primary_pass(capacity, follow, refs):
    plan_ref, fetched_ref, points_ref, other_ref, both_ref, lhs_ref = refs
    segs = plan_ref.shape[1]

    def first(s, i):
        stage_a(s, plan_ref[0, s], capacity, fetched_ref, points_ref, both_ref, lhs_ref, i)

    def second(s, i):
        sums = sums_of(both_ref, lhs_ref, i)
        other_ref[s] = sums * (1.0 / sums[6:7])

    for i in range(WIDE):
        first(i, i)

    def one_group(g, last):
        base = g * (2 * WIDE)
        for i in range(WIDE):
            second(base + i, i)
            first(base + WIDE + i, WIDE + i)
        for i in range(WIDE):
            second(base + WIDE + i, WIDE + i)
            if last:
                follow(i)
            else:
                first(base + 2 * WIDE + i, i)

    groups = segs // (2 * WIDE)

    def full_group(g, carry):
        one_group(g, False)
        return carry

    lax.fori_loop(0, groups - 1, full_group, 0)
    one_group(groups - 1, True)


def secondary_pass(step, apart, base_row, low, end, sets, refs):
    plan_ref, count_ref, fetched_ref, points_ref, weights_ref, other_ref = refs[:6]
    out_ref, both_ref, lhs_ref, left_ref = refs[6:]

    def entry(row, place):
        return plan_ref[row, jnp.minimum(low + place, end - 1)]

    def first(place, i):
        s, start = entry(1, place), entry(2, place)
        stage_a(s, start, step, fetched_ref, points_ref, both_ref, lhs_ref, i)

    def second(place, i):
        s = entry(1, place)
        sums = sums_of(both_ref, lhs_ref, i)
        inverse = 1.0 / sums[6:7]
        weights = weights_ref[pl.ds(s, 1), :]
        position = lax.broadcasted_iota(jnp.int32, weights.shape, 1)
        weights = jnp.where(position < count_ref[s], weights, 0.0)
        gap = (weights * inverse) * (sums * inverse - other_ref[s])
        high = gap.astype(jnp.bfloat16).astype(jnp.float32)
        left_ref[i] = jnp.concatenate([high, gap - high], axis=0).astype(jnp.bfloat16)

    def third(place, i):
        left, both = left_ref[i], both_ref[i]
        half = both.shape[0] // 2
        if i % 2 == 0:
            result = dot_last(left, both)
            result = result[:8] + result[8:]
            result = result[:, :half] + result[:, half:]
        else:
            result = dot_last(both, left)
            result = (result[:half] + result[half:]).T
            result = result[:8] + result[8:]
        out_ref[pl.ds(entry(base_row, place), 3, stride=apart), :] = result[3:6]

    def begin(i):
        if i < 2 * sets:
            first(i, i)

    def one_group(g, last):
        base = g * (3 * sets)
        for phase in range(3):
            for i in range(sets):
                a, b, c = (phase * sets + sets * t + i for t in (2, 1, 0))
                third(base + c, c)
                if not last or b < 3 * sets:
                    second(base + b, b % (3 * sets))
                if not last or a < 3 * sets:
                    first(base + a, a % (3 * sets))

    def finish():
        for i in range(sets):
            second(i, i)
        groups = (end - low + 3 * sets - 1) // (3 * sets)

        def full_group(g, carry):
            one_group(g, False)
            return carry

        lax.fori_loop(0, groups - 1, full_group, 0)
        one_group(groups - 1, True)

    return begin, finish


def early_kernel(capacity, plan_ref, count_ref, fetched_ref, points_ref, far_weights_ref, *refs):
    far_other_ref, out_ref, both_ref, lhs_ref, left_ref, other_ref, weights_ref, sems = refs
    load = pltpu.make_async_copy(far_weights_ref, weights_ref, sems.at[0])
    store = pltpu.make_async_copy(other_ref, far_other_ref, sems.at[1])
    load.start()
    out_ref[...] = jnp.zeros_like(out_ref)
    begin, finish = secondary_pass(
        1,
        1,
        5,
        0,
        plan_ref[4, 0],
        EARLY_SETS,
        (plan_ref, count_ref, fetched_ref, points_ref, weights_ref, other_ref)
        + (out_ref, both_ref, lhs_ref, left_ref),
    )
    primary_pass(
        capacity, begin, (plan_ref, fetched_ref, points_ref, other_ref, both_ref, lhs_ref)
    )
    store.start()
    load.wait()
    finish()
    store.wait()


def late_kernel(capacity, plan_ref, count_ref, fetched_ref, points_ref, *refs):
    far_weights_ref, far_other_ref, before_ref, out_ref = refs[:4]
    both_ref, lhs_ref, left_ref, other_ref, weights_ref, sems = refs[4:]
    loads = [
        pltpu.make_async_copy(far_other_ref, other_ref, sems.at[0]),
        pltpu.make_async_copy(far_weights_ref, weights_ref, sems.at[1]),
    ]
    for load in loads:
        load.start()
    out_ref[...] = jnp.zeros_like(out_ref)
    for row in range(0, before_ref.shape[0], 8):
        out_ref[pl.ds(row * capacity, 8, stride=capacity), :] = before_ref[row : row + 8, :]

    begin, finish = secondary_pass(
        capacity - 1,
        capacity,
        3,
        plan_ref[4, 0],
        plan_ref.shape[1],
        LATE_SETS,
        (plan_ref, count_ref, fetched_ref, points_ref, weights_ref, other_ref)
        + (out_ref, both_ref, lhs_ref, left_ref),
    )
    for i in range(2 * LATE_SETS):
        begin(i)
    for load in loads:
        load.wait()
    finish()


def assemble_kernel(capacity, blocks, ids_ref, in_ref, out_ref):
    devices = ids_ref.shape[1]
    block = lax.broadcasted_iota(jnp.int32, (blocks, devices), 0)
    select, rows = [], []
    for rank in range(capacity):
        select.append(jnp.where(block == ids_ref[rank : rank + 1, :], 1.0, 0.0))
        step = 3 * capacity
        parts = [in_ref[pl.ds(c * capacity + rank, devices, stride=step), :] for c in range(3)]
        rows.append(jnp.concatenate(parts, axis=1))
    select = jnp.concatenate(select, axis=1).astype(jnp.bfloat16)
    total = None
    for piece in pieces(jnp.concatenate(rows, axis=0)):
        term = jnp.dot(select, piece.astype(jnp.bfloat16), preferred_element_type=jnp.float32)
        total = term if total is None else total + term
    nodes = in_ref.shape[1]
    for c in range(3):
        out_ref[c * blocks : (c + 1) * blocks, :] = total[:, c * nodes : (c + 1) * nodes]


def body(node_coords, node_disp, qpoints, qweights, qcount, sec_block, pri_block):
    devices = lax.axis_size("gx") * lax.axis_size("gy")
    blocks = node_coords.shape[0]
    nodes = node_coords.shape[2]
    segs = qpoints.shape[0]
    quad = qpoints.shape[2]
    slots = 2 * segs
    cap = slots // devices
    f32 = jnp.float32
    smem = pl.BlockSpec(memory_space=pltpu.SMEM)
    vmem = pl.BlockSpec(memory_space=pltpu.VMEM)

    limit = pltpu.CompilerParams(vmem_limit_bytes=16 * 1024 * 1024)

    def near(value):
        return pltpu.with_memory_space_constraint(value, pltpu.VMEM)

    def far(value):
        return pltpu.with_memory_space_constraint(value, pltpu.HBM)

    def exchange(value):
        return lax.all_to_all(value, AXES, split_axis=0, concat_axis=0, tiled=True)

    plan, request = pl.pallas_call(
        functools.partial(plan_kernel, devices, cap, blocks),
        out_shape=(
            jax.ShapeDtypeStruct((8, segs), jnp.int32),
            jax.ShapeDtypeStruct((devices, 128), f32),
        ),
        in_specs=[vmem, vmem],
        out_specs=(vmem, vmem),
        compiler_params=limit,
    )(far(sec_block.reshape(1, segs)), far(pri_block.reshape(1, segs)))
    xc = jnp.transpose(node_coords, (1, 0, 2)).reshape(3 * blocks, nodes)
    xu = jnp.transpose(node_disp, (1, 0, 2)).reshape(3 * blocks, nodes)
    hbm = pl.BlockSpec(memory_space=pltpu.HBM)
    table = pl.pallas_call(
        table_kernel,
        out_shape=pltpu.VMEM((8 * blocks, nodes), f32),
        in_specs=[vmem, vmem],
        out_specs=vmem,
        compiler_params=limit,
    )(far(xc), far(xu))
    received = exchange(request.reshape(devices, 1, 128)).reshape(devices, 128)

    def gather(first, rows):
        out, turned = pl.pallas_call(
            functools.partial(gather_kernel, devices, cap, first),
            out_shape=(
                pltpu.HBM((devices * rows, nodes), f32),
                jax.ShapeDtypeStruct((2 * cap, devices), jnp.int32),
            ),
            in_specs=[vmem, vmem],
            out_specs=(hbm, vmem),
            scratch_shapes=[
                pltpu.VMEM((devices * rows, nodes), f32),
                pltpu.SMEM((2 * cap, devices), jnp.int32),
                pltpu.SemaphoreType.DMA,
                pltpu.SemaphoreType.DMA((CHUNKS,)),
            ],
            compiler_params=limit,
        )(received, near(table))
        return out.reshape(devices, rows // 2, 2, nodes), turned

    out1, turned = gather(True, 6 * cap + 6)
    out2, _ = gather(False, 6 * cap - 6)
    in1 = near(exchange(out1).reshape(-1, nodes))
    in2 = near(exchange(out2).reshape(-1, nodes))
    points = pl.pallas_call(
        pack_kernel,
        out_shape=pltpu.VMEM((quad // 128, segs * 8, 128), f32),
        in_specs=[vmem],
        out_specs=vmem,
        compiler_params=limit,
    )(jnp.transpose(qpoints, (1, 0, 2)))
    points = near(points)

    def scratch(count, sems):
        return [
            pltpu.VMEM((count, 2 * nodes, quad), jnp.bfloat16),
            pltpu.VMEM((count, 16, 2 * nodes), jnp.bfloat16),
            pltpu.VMEM((count, 16, quad), jnp.bfloat16),
            pltpu.VMEM((segs, 8, quad), f32),
            pltpu.VMEM((segs, quad), f32),
            pltpu.SemaphoreType.DMA((sems,)),
        ]

    weights = far(qweights)
    other, parcels = pl.pallas_call(
        functools.partial(early_kernel, cap),
        out_shape=(
            pltpu.HBM((segs, 8, quad), f32),
            jax.ShapeDtypeStruct((devices * 3, nodes), f32),
        ),
        in_specs=[smem, smem, vmem, vmem, hbm],
        out_specs=(hbm, vmem),
        scratch_shapes=scratch(max(2 * WIDE, 3 * EARLY_SETS), 2),
        compiler_params=limit,
    )(plan, qcount, in1, points, weights)
    parcels = pl.pallas_call(
        functools.partial(late_kernel, cap),
        out_shape=pltpu.VMEM((devices * 3 * cap, nodes), f32),
        in_specs=[smem, smem, vmem, vmem, hbm, hbm, vmem],
        out_specs=vmem,
        scratch_shapes=scratch(3 * LATE_SETS, 2),
        compiler_params=limit,
    )(plan, qcount, in2, points, weights, far(other), parcels)
    incoming = exchange(parcels.reshape(devices, 3, cap, nodes)).reshape(-1, nodes)
    gap = pl.pallas_call(
        functools.partial(assemble_kernel, cap, blocks),
        out_shape=jax.ShapeDtypeStruct((3 * blocks, nodes), f32),
        in_specs=[vmem, vmem],
        out_specs=vmem,
        compiler_params=limit,
    )(turned, near(incoming))
    return jnp.transpose(gap.reshape(3, blocks, nodes), (1, 0, 2))


def solution(mesh):
    split3 = P(AXES, None, None)
    placed = (split3, split3, split3, P(AXES, None), P(AXES), P(AXES), P(AXES))
    return jax.shard_map(body, mesh=mesh, in_specs=placed, out_specs=split3, check_vma=False)
```

```python
import functools
import jax
import jax.numpy as jnp
from jax import lax
from jax.experimental import pallas as pl
from jax.experimental.pallas import tpu as pltpu
from jax.sharding import PartitionSpec as P

AXES = ("gx", "gy")
WIDE = 16
EARLY_SETS = 7
LATE_SETS = 8
CHUNKS = 4


def strict_upper(size):
    row = lax.broadcasted_iota(jnp.int32, (size, size), 0)
    column = lax.broadcasted_iota(jnp.int32, (size, size), 1)
    return jnp.where(row < column, 1.0, 0.0).astype(jnp.bfloat16)


def dot_last(left, right):
    return lax.dot_general(
        left, right, (((1,), (1,)), ((), ())), preferred_element_type=jnp.float32
    )


def route_kernel(devices, capacity, blocks, sec_ref, pri_ref, request_ref, route_ref):
    segs = sec_ref.shape[1]
    upper = strict_upper(segs)
    device = lax.broadcasted_iota(jnp.int32, (devices, segs), 0).astype(jnp.float32)
    column = lax.broadcasted_iota(jnp.int32, (request_ref.shape[1], segs), 0).astype(jnp.float32)
    request = jnp.zeros(request_ref.shape, jnp.float32)
    for side, ref in enumerate((sec_ref, pri_ref)):
        ids = ref[...].astype(jnp.float32)
        owner = jnp.floor((ids + 0.5) * (1.0 / blocks))
        local = ids - owner * blocks
        mine = jnp.where(device == owner, 1.0, 0.0)
        narrow = mine.astype(jnp.bfloat16)
        before = jnp.dot(narrow, upper, preferred_element_type=jnp.float32)
        rank = jnp.sum(mine * before, axis=0, keepdims=True)
        coarse = jnp.floor(local * (1.0 / 16.0)) * 16.0
        here = column == rank + side * capacity
        for part in (coarse, local - coarse):
            request += dot_last(narrow, jnp.where(here, 8.0 * part, 0.0).astype(jnp.bfloat16))
        route_ref[2 * side : 2 * side + 1, :] = owner
        route_ref[2 * side + 1 : 2 * side + 2, :] = rank
    request_ref[...] = request


def order_kernel(capacity, route_ref, plan_ref):
    segs = route_ref.shape[1]
    upper = strict_upper(segs)
    sec_owner, sec_rank = route_ref[0:1, :], route_ref[1:2, :]
    pri_owner, pri_rank = route_ref[2:3, :], route_ref[3:4, :]
    early = jnp.where(sec_rank == 0.0, 1.0, 0.0)
    spread = jnp.broadcast_to(early, (16, segs)).astype(jnp.bfloat16)
    ahead = jnp.dot(spread, upper, preferred_element_type=jnp.float32)[:1]
    count = jnp.sum(early, axis=1, keepdims=True)
    number = lax.broadcasted_iota(jnp.int32, (1, segs), 1).astype(jnp.float32)
    place = jnp.where(sec_rank == 0.0, ahead, count + number - ahead)
    target = lax.broadcasted_iota(jnp.int32, (segs, segs), 0).astype(jnp.float32)
    moved = jnp.where(target == place, 1.0, 0.0).astype(jnp.bfloat16)
    row = lax.broadcasted_iota(jnp.int32, (16, segs), 0)
    values = jnp.where(row == 0, number, jnp.where(row == 1, sec_owner, sec_rank))
    values = dot_last(values.astype(jnp.bfloat16), moved)
    seg, dev, rank = values[0:1], values[1:2], values[2:3]
    start = jnp.where(
        rank == 0.0,
        dev * (6 * capacity + 6) + 6 * capacity,
        dev * (6 * capacity - 6) + (rank - 1.0),
    )
    rows = (
        pri_owner * (6 * capacity + 6) + pri_rank,
        seg,
        start,
        dev * (3 * capacity) + rank,
        jnp.broadcast_to(count, (1, segs)),
        dev * 3.0,
    )
    plan_ref[...] = jnp.zeros_like(plan_ref)
    for i, value in enumerate(rows):
        plan_ref[i : i + 1, :] = value.astype(jnp.int32)


def table_kernel(xc_ref, xu_ref, out_ref):
    blocks = xc_ref.shape[0] // 3

    def one_block(b, carry):
        for half, ref in enumerate((xc_ref, xu_ref)):
            for c in range(3):
                here = pl.ds(pl.multiple_of(c * blocks + b * 8, 8), 8)
                out_ref[pl.ds(b * 64 + 3 * half + c, 8, stride=8), :] = ref[here, :]
        return carry

    lax.fori_loop(0, blocks // 8, one_block, 0, unroll=4)


def gather_kernel(devices, capacity, first, ids_ref, table_ref, *refs):
    far_ref, turned_ref, near_ref, local_ref, sem, sems = refs
    turned_ref[...] = ids_ref[...].T[: 2 * capacity].astype(jnp.int32)
    copy = pltpu.make_async_copy(turned_ref, local_ref, sem)
    copy.start()
    copy.wait()
    if first:
        parts = [(1, rank, rank, capacity) for rank in range(capacity)]
        parts.append((0, 0, 6 * capacity, 1))
    else:
        parts = [(0, rank, rank - 1, capacity - 1) for rank in range(1, capacity)]
    rows = 6 * len(parts)

    def one_device(dev, carry):
        for side, rank, start, step in parts:
            row = pl.multiple_of(local_ref[side * capacity + rank, dev], 8)
            patch = table_ref[pl.ds(row, 8), :]
            near_ref[pl.ds(dev * rows + start, 6, stride=step), :] = patch[:6]
        return carry

    part = devices // CHUNKS
    stores = []
    for chunk in range(CHUNKS):
        lax.fori_loop(chunk * part, (chunk + 1) * part, one_device, 0, unroll=4)
        here = pl.ds(chunk * part * rows, part * rows)
        stores.append(pltpu.make_async_copy(near_ref.at[here], far_ref.at[here], sems.at[chunk]))
        stores[-1].start()
    for store in stores:
        store.wait()


def pack_kernel(points_ref, out_ref):
    rows = 8
    segs = points_ref.shape[1]
    out_ref[...] = jnp.zeros_like(out_ref)

    def one_block(b, carry):
        here = pl.ds(pl.multiple_of(b * rows, rows), rows)
        x, y, z = points_ref[0, here], points_ref[1, here], points_ref[2, here]
        square = 1.0 + 2.0 * (x * x + y * y + z * z)
        for row, value in enumerate((x, y, z, jnp.ones_like(x), square)):
            for half in range(x.shape[1] // 128):
                lanes = slice(half * 128, half * 128 + 128)
                out_ref[half, pl.ds(b * rows * rows + row, rows, stride=rows), :] = value[:, lanes]
        return carry

    lax.fori_loop(0, segs // rows, one_block, 0, unroll=2)


def pieces(value):
    first = value.astype(jnp.bfloat16).astype(jnp.float32)
    rest = value - first
    second = rest.astype(jnp.bfloat16).astype(jnp.float32)
    return (first, second, rest - second)


def node_side(fetched_ref, start, step):
    raw = fetched_ref[pl.ds(start, 6, stride=step), :]
    raw = jnp.concatenate([raw, jnp.zeros((2, raw.shape[1]), jnp.float32)], axis=0)
    row = lax.broadcasted_iota(jnp.int32, raw.shape, 0)
    coord = jnp.where(row < 3, raw, 0.0)
    square = 2.0 * jnp.sum(coord * coord, axis=0, keepdims=True)
    extended = jnp.where(row == 3, square, jnp.where(row == 4, 1.0, -4.0 * coord))
    a, b, c = pieces(extended)
    stacked = jnp.concatenate([a, a, b, b, a, c], axis=0)
    disp = jnp.where(row < 3, 0.0, jnp.where(row == 6, 1.0, raw))
    high = disp.astype(jnp.bfloat16).astype(jnp.float32)
    lhs = jnp.concatenate([high, disp - high], axis=0)
    lhs = jnp.concatenate([lhs, lhs], axis=1).astype(jnp.bfloat16)
    return stacked.astype(jnp.bfloat16).T, lhs


def points_of(points_ref, s):
    here = pl.ds(pl.multiple_of(s * 8, 8), 8)
    return jnp.concatenate([points_ref[h, here] for h in range(points_ref.shape[0])], axis=1)


def point_side(points):
    a, b, c = pieces(points)
    return jnp.concatenate([a, b, a, b, c, a], axis=0).astype(jnp.bfloat16)


def kernel_values(node_op, point_op):
    dist = jnp.dot(node_op, point_op, preferred_element_type=jnp.float32)
    value = 1.0 / dist
    high = value.astype(jnp.bfloat16)
    low = (value - high.astype(jnp.float32)).astype(jnp.bfloat16)
    return jnp.concatenate([high, low], axis=0)


def stage_a(s, start, step, fetched_ref, points_ref, both_ref, lhs_ref, i):
    node_op, lhs = node_side(fetched_ref, start, step)
    lhs_ref[i] = lhs
    both_ref[i] = kernel_values(node_op, point_side(points_of(points_ref, s)))


def sums_of(both_ref, lhs_ref, i):
    sums = jnp.dot(lhs_ref[i], both_ref[i], preferred_element_type=jnp.float32)
    return sums[:8] + sums[8:]


def primary_pass(capacity, follow, refs):
    plan_ref, fetched_ref, points_ref, other_ref, both_ref, lhs_ref = refs
    segs = plan_ref.shape[1]

    def first(s, i):
        stage_a(s, plan_ref[0, s], capacity, fetched_ref, points_ref, both_ref, lhs_ref, i)

    def second(s, i):
        sums = sums_of(both_ref, lhs_ref, i)
        other_ref[s] = sums * (1.0 / sums[6:7])

    for i in range(WIDE):
        first(i, i)

    def one_group(g, last):
        base = g * (2 * WIDE)
        for i in range(WIDE):
            second(base + i, i)
            first(base + WIDE + i, WIDE + i)
        for i in range(WIDE):
            second(base + WIDE + i, WIDE + i)
            if last:
                follow(i)
            else:
                first(base + 2 * WIDE + i, i)

    groups = segs // (2 * WIDE)

    def full_group(g, carry):
        one_group(g, False)
        return carry

    lax.fori_loop(0, groups - 1, full_group, 0)
    one_group(groups - 1, True)


def secondary_pass(step, apart, base_row, low, end, sets, refs):
    plan_ref, count_ref, fetched_ref, points_ref, weights_ref, other_ref = refs[:6]
    out_ref, both_ref, lhs_ref, left_ref = refs[6:]

    def entry(row, place):
        return plan_ref[row, jnp.minimum(low + place, end - 1)]

    def first(place, i):
        s, start = entry(1, place), entry(2, place)
        stage_a(s, start, step, fetched_ref, points_ref, both_ref, lhs_ref, i)

    def second(place, i):
        s = entry(1, place)
        sums = sums_of(both_ref, lhs_ref, i)
        inverse = 1.0 / sums[6:7]
        weights = weights_ref[pl.ds(s, 1), :]
        position = lax.broadcasted_iota(jnp.int32, weights.shape, 1)
        weights = jnp.where(position < count_ref[s], weights, 0.0)
        gap = (weights * inverse) * (sums * inverse - other_ref[s])
        high = gap.astype(jnp.bfloat16).astype(jnp.float32)
        left_ref[i] = jnp.concatenate([high, gap - high], axis=0).astype(jnp.bfloat16)

    def third(place, i):
        left, both = left_ref[i], both_ref[i]
        half = both.shape[0] // 2
        if i % 2 == 0:
            result = dot_last(left, both)
            result = result[:8] + result[8:]
            result = result[:, :half] + result[:, half:]
        else:
            result = dot_last(both, left)
            result = (result[:half] + result[half:]).T
            result = result[:8] + result[8:]
        out_ref[pl.ds(entry(base_row, place), 3, stride=apart), :] = result[3:6]

    def begin(i):
        if i < 2 * sets:
            first(i, i)

    def one_group(g, last):
        base = g * (3 * sets)
        for phase in range(3):
            for i in range(sets):
                a, b, c = (phase * sets + sets * t + i for t in (2, 1, 0))
                third(base + c, c)
                if not last or b < 3 * sets:
                    second(base + b, b % (3 * sets))
                if not last or a < 3 * sets:
                    first(base + a, a % (3 * sets))

    def finish():
        for i in range(sets):
            second(i, i)
        groups = (end - low + 3 * sets - 1) // (3 * sets)

        def full_group(g, carry):
            one_group(g, False)
            return carry

        lax.fori_loop(0, groups - 1, full_group, 0)
        one_group(groups - 1, True)

    return begin, finish


def early_kernel(capacity, plan_ref, count_ref, fetched_ref, points_ref, far_weights_ref, *refs):
    far_other_ref, out_ref, both_ref, lhs_ref, left_ref, other_ref, weights_ref, sems = refs
    load = pltpu.make_async_copy(far_weights_ref, weights_ref, sems.at[0])
    store = pltpu.make_async_copy(other_ref, far_other_ref, sems.at[1])
    load.start()
    out_ref[...] = jnp.zeros_like(out_ref)
    begin, finish = secondary_pass(
        1,
        1,
        5,
        0,
        plan_ref[4, 0],
        EARLY_SETS,
        (plan_ref, count_ref, fetched_ref, points_ref, weights_ref, other_ref)
        + (out_ref, both_ref, lhs_ref, left_ref),
    )
    primary_pass(
        capacity, begin, (plan_ref, fetched_ref, points_ref, other_ref, both_ref, lhs_ref)
    )
    store.start()
    load.wait()
    finish()
    store.wait()


def late_kernel(capacity, plan_ref, count_ref, fetched_ref, points_ref, *refs):
    far_weights_ref, far_other_ref, before_ref, out_ref = refs[:4]
    both_ref, lhs_ref, left_ref, other_ref, weights_ref, sems = refs[4:]
    loads = [
        pltpu.make_async_copy(far_other_ref, other_ref, sems.at[0]),
        pltpu.make_async_copy(far_weights_ref, weights_ref, sems.at[1]),
    ]
    for load in loads:
        load.start()
    out_ref[...] = jnp.zeros_like(out_ref)
    for row in range(0, before_ref.shape[0], 8):
        out_ref[pl.ds(row * capacity, 8, stride=capacity), :] = before_ref[row : row + 8, :]

    begin, finish = secondary_pass(
        capacity - 1,
        capacity,
        3,
        plan_ref[4, 0],
        plan_ref.shape[1],
        LATE_SETS,
        (plan_ref, count_ref, fetched_ref, points_ref, weights_ref, other_ref)
        + (out_ref, both_ref, lhs_ref, left_ref),
    )
    for i in range(2 * LATE_SETS):
        begin(i)
    for load in loads:
        load.wait()
    finish()


def assemble_kernel(capacity, blocks, ids_ref, in_ref, out_ref, near_ref, sems):
    devices = ids_ref.shape[1]
    block = 8 * lax.broadcasted_iota(jnp.int32, (blocks, devices), 0)
    nodes = in_ref.shape[1]
    select = [
        jnp.where(block == ids_ref[rank : rank + 1, :], 1.0, 0.0) for rank in range(capacity)
    ]
    select = jnp.concatenate(select, axis=1).astype(jnp.bfloat16)
    step = 3 * capacity
    stores = []
    for components in ((0, 1), (2,)):
        rows = []
        for rank in range(capacity):
            parts = [
                in_ref[pl.ds(c * capacity + rank, devices, stride=step), :] for c in components
            ]
            rows.append(jnp.concatenate(parts, axis=1))
        total = None
        for piece in pieces(jnp.concatenate(rows, axis=0)):
            term = jnp.dot(select, piece.astype(jnp.bfloat16), preferred_element_type=jnp.float32)
            total = term if total is None else total + term
        for i, c in enumerate(components):
            near_ref[c * blocks : (c + 1) * blocks, :] = total[:, i * nodes : (i + 1) * nodes]
        here = pl.ds(components[0] * blocks, len(components) * blocks)
        stores.append(
            pltpu.make_async_copy(near_ref.at[here], out_ref.at[here], sems.at[len(stores)])
        )
        stores[-1].start()
    for store in stores:
        store.wait()


def body(node_coords, node_disp, qpoints, qweights, qcount, sec_block, pri_block):
    devices = lax.axis_size("gx") * lax.axis_size("gy")
    blocks = node_coords.shape[0]
    nodes = node_coords.shape[2]
    segs = qpoints.shape[0]
    quad = qpoints.shape[2]
    slots = 2 * segs
    cap = slots // devices
    f32 = jnp.float32
    smem = pl.BlockSpec(memory_space=pltpu.SMEM)
    vmem = pl.BlockSpec(memory_space=pltpu.VMEM)

    limit = pltpu.CompilerParams(vmem_limit_bytes=16 * 1024 * 1024)

    def near(value):
        return pltpu.with_memory_space_constraint(value, pltpu.VMEM)

    def far(value):
        return pltpu.with_memory_space_constraint(value, pltpu.HBM)

    def exchange(value):
        return lax.all_to_all(value, AXES, split_axis=0, concat_axis=0, tiled=True)

    request, route = pl.pallas_call(
        functools.partial(route_kernel, devices, cap, blocks),
        out_shape=(jax.ShapeDtypeStruct((devices, 128), f32), jax.ShapeDtypeStruct((4, segs), f32)),
        in_specs=[vmem, vmem],
        out_specs=(vmem, vmem),
        compiler_params=limit,
    )(far(sec_block.reshape(1, segs)), far(pri_block.reshape(1, segs)))
    plan = pl.pallas_call(
        functools.partial(order_kernel, cap),
        out_shape=jax.ShapeDtypeStruct((8, segs), jnp.int32),
        in_specs=[vmem],
        out_specs=vmem,
        compiler_params=limit,
    )(route)
    xc = jnp.transpose(node_coords, (1, 0, 2)).reshape(3 * blocks, nodes)
    xu = jnp.transpose(node_disp, (1, 0, 2)).reshape(3 * blocks, nodes)
    hbm = pl.BlockSpec(memory_space=pltpu.HBM)
    table = pl.pallas_call(
        table_kernel,
        out_shape=pltpu.VMEM((8 * blocks, nodes), f32),
        in_specs=[vmem, vmem],
        out_specs=vmem,
        compiler_params=limit,
    )(far(xc), far(xu))
    received = exchange(request.reshape(devices, 1, 128)).reshape(devices, 128)

    def gather(first, rows):
        out, turned = pl.pallas_call(
            functools.partial(gather_kernel, devices, cap, first),
            out_shape=(
                pltpu.HBM((devices * rows, nodes), f32),
                jax.ShapeDtypeStruct((2 * cap, devices), jnp.int32),
            ),
            in_specs=[vmem, vmem],
            out_specs=(hbm, vmem),
            scratch_shapes=[
                pltpu.VMEM((devices * rows, nodes), f32),
                pltpu.SMEM((2 * cap, devices), jnp.int32),
                pltpu.SemaphoreType.DMA,
                pltpu.SemaphoreType.DMA((CHUNKS,)),
            ],
            compiler_params=limit,
        )(received, near(table))
        return out.reshape(devices, rows // 2, 2, nodes), turned

    out1, turned = gather(True, 6 * cap + 6)
    out2, _ = gather(False, 6 * cap - 6)
    in1 = near(exchange(out1).reshape(-1, nodes))
    in2 = near(exchange(out2).reshape(-1, nodes))
    points = pl.pallas_call(
        pack_kernel,
        out_shape=pltpu.VMEM((quad // 128, segs * 8, 128), f32),
        in_specs=[vmem],
        out_specs=vmem,
        compiler_params=limit,
    )(jnp.transpose(qpoints, (1, 0, 2)))
    points = near(points)

    def scratch(count, sems):
        return [
            pltpu.VMEM((count, 2 * nodes, quad), jnp.bfloat16),
            pltpu.VMEM((count, 16, 2 * nodes), jnp.bfloat16),
            pltpu.VMEM((count, 16, quad), jnp.bfloat16),
            pltpu.VMEM((segs, 8, quad), f32),
            pltpu.VMEM((segs, quad), f32),
            pltpu.SemaphoreType.DMA((sems,)),
        ]

    weights = far(qweights)
    other, parcels = pl.pallas_call(
        functools.partial(early_kernel, cap),
        out_shape=(
            pltpu.HBM((segs, 8, quad), f32),
            jax.ShapeDtypeStruct((devices * 3, nodes), f32),
        ),
        in_specs=[smem, smem, vmem, vmem, hbm],
        out_specs=(hbm, vmem),
        scratch_shapes=scratch(max(2 * WIDE, 3 * EARLY_SETS), 2),
        compiler_params=limit,
    )(plan, qcount, in1, points, weights)
    parcels = pl.pallas_call(
        functools.partial(late_kernel, cap),
        out_shape=pltpu.VMEM((devices * 3 * cap, nodes), f32),
        in_specs=[smem, smem, vmem, vmem, hbm, hbm, vmem],
        out_specs=vmem,
        scratch_shapes=scratch(3 * LATE_SETS, 2),
        compiler_params=limit,
    )(plan, qcount, in2, points, weights, far(other), parcels)
    incoming = exchange(parcels.reshape(devices, 3, cap, nodes)).reshape(-1, nodes)
    gap = pl.pallas_call(
        functools.partial(assemble_kernel, cap, blocks),
        out_shape=jax.ShapeDtypeStruct((3 * blocks, nodes), f32),
        in_specs=[vmem, vmem],
        out_specs=hbm,
        scratch_shapes=[
            pltpu.VMEM((3 * blocks, nodes), f32),
            pltpu.SemaphoreType.DMA((2,)),
        ],
        compiler_params=limit,
    )(turned, near(incoming))
    return jnp.transpose(gap.reshape(3, blocks, nodes), (1, 0, 2))


def solution(mesh):
    split3 = P(AXES, None, None)
    placed = (split3, split3, split3, P(AXES, None), P(AXES), P(AXES), P(AXES))
    return jax.shard_map(body, mesh=mesh, in_specs=placed, out_specs=split3, check_vma=False)
```

```python
import functools
import jax
import jax.numpy as jnp
from jax import lax
from jax.experimental import pallas as pl
from jax.experimental.pallas import tpu as pltpu
from jax.sharding import PartitionSpec as P

AXES = ("gx", "gy")
WIDE = 16
EARLY_SETS = 7
LATE_SETS = 8
CHUNKS = 4


def strict_upper(size):
    row = lax.broadcasted_iota(jnp.int32, (size, size), 0)
    column = lax.broadcasted_iota(jnp.int32, (size, size), 1)
    return jnp.where(row < column, 1.0, 0.0).astype(jnp.bfloat16)


def dot_last(left, right):
    return lax.dot_general(
        left, right, (((1,), (1,)), ((), ())), preferred_element_type=jnp.float32
    )


def route_kernel(devices, capacity, blocks, sec_ref, pri_ref, request_ref, route_ref):
    segs = sec_ref.shape[1]
    upper = strict_upper(segs)
    device = lax.broadcasted_iota(jnp.int32, (devices, segs), 0).astype(jnp.float32)
    column = lax.broadcasted_iota(jnp.int32, (request_ref.shape[1], segs), 0).astype(jnp.float32)
    request = jnp.zeros(request_ref.shape, jnp.float32)
    for side, ref in enumerate((sec_ref, pri_ref)):
        ids = ref[...].astype(jnp.float32)
        owner = jnp.floor((ids + 0.5) * (1.0 / blocks))
        local = ids - owner * blocks
        mine = jnp.where(device == owner, 1.0, 0.0)
        narrow = mine.astype(jnp.bfloat16)
        before = jnp.dot(narrow, upper, preferred_element_type=jnp.float32)
        rank = jnp.sum(mine * before, axis=0, keepdims=True)
        coarse = jnp.floor(local * (1.0 / 16.0)) * 16.0
        here = column == rank + side * capacity
        for part in (coarse, local - coarse):
            request += dot_last(narrow, jnp.where(here, 8.0 * part, 0.0).astype(jnp.bfloat16))
        route_ref[2 * side : 2 * side + 1, :] = owner
        route_ref[2 * side + 1 : 2 * side + 2, :] = rank
    request_ref[...] = request


def order_kernel(capacity, route_ref, plan_ref):
    segs = route_ref.shape[1]
    upper = strict_upper(segs)
    sec_owner, sec_rank = route_ref[0:1, :], route_ref[1:2, :]
    pri_owner, pri_rank = route_ref[2:3, :], route_ref[3:4, :]
    early = jnp.where(sec_rank == 0.0, 1.0, 0.0)
    spread = jnp.broadcast_to(early, (16, segs)).astype(jnp.bfloat16)
    ahead = jnp.dot(spread, upper, preferred_element_type=jnp.float32)[:1]
    count = jnp.sum(early, axis=1, keepdims=True)
    number = lax.broadcasted_iota(jnp.int32, (1, segs), 1).astype(jnp.float32)
    place = jnp.where(sec_rank == 0.0, ahead, count + number - ahead)
    target = lax.broadcasted_iota(jnp.int32, (segs, segs), 0).astype(jnp.float32)
    moved = jnp.where(target == place, 1.0, 0.0).astype(jnp.bfloat16)
    row = lax.broadcasted_iota(jnp.int32, (16, segs), 0)
    values = jnp.where(row == 0, number, jnp.where(row == 1, sec_owner, sec_rank))
    values = dot_last(values.astype(jnp.bfloat16), moved)
    seg, dev, rank = values[0:1], values[1:2], values[2:3]
    start = jnp.where(
        rank == 0.0,
        dev * (6 * capacity + 6) + 6 * capacity,
        dev * (6 * capacity - 6) + (rank - 1.0),
    )
    rows = (
        pri_owner * (6 * capacity + 6) + pri_rank,
        seg,
        start,
        dev * (3 * capacity) + rank,
        jnp.broadcast_to(count, (1, segs)),
        dev * 3.0,
    )
    plan_ref[...] = jnp.zeros_like(plan_ref)
    for i, value in enumerate(rows):
        plan_ref[i : i + 1, :] = value.astype(jnp.int32)


def table_kernel(xc_ref, xu_ref, out_ref):
    blocks = xc_ref.shape[0] // 3

    def one_block(b, carry):
        for half, ref in enumerate((xc_ref, xu_ref)):
            for c in range(3):
                here = pl.ds(pl.multiple_of(c * blocks + b * 8, 8), 8)
                out_ref[pl.ds(b * 64 + 3 * half + c, 8, stride=8), :] = ref[here, :]
        return carry

    lax.fori_loop(0, blocks // 8, one_block, 0, unroll=4)


def gather_kernel(devices, capacity, first, ids_ref, table_ref, *refs):
    far_ref, turned_ref, near_ref, local_ref, sem, sems = refs
    turned_ref[...] = ids_ref[...].T[: 2 * capacity].astype(jnp.int32)
    copy = pltpu.make_async_copy(turned_ref, local_ref, sem)
    copy.start()
    copy.wait()
    if first:
        parts = [(1, rank, rank, capacity) for rank in range(capacity)]
        parts.append((0, 0, 6 * capacity, 1))
    else:
        parts = [(0, rank, rank - 1, capacity - 1) for rank in range(1, capacity)]
    rows = 6 * len(parts)

    def one_device(dev, carry):
        for side, rank, start, step in parts:
            row = pl.multiple_of(local_ref[side * capacity + rank, dev], 8)
            patch = table_ref[pl.ds(row, 8), :]
            near_ref[pl.ds(dev * rows + start, 6, stride=step), :] = patch[:6]
        return carry

    part = devices // CHUNKS
    stores = []
    for chunk in range(CHUNKS):
        lax.fori_loop(chunk * part, (chunk + 1) * part, one_device, 0, unroll=4)
        here = pl.ds(chunk * part * rows, part * rows)
        stores.append(pltpu.make_async_copy(near_ref.at[here], far_ref.at[here], sems.at[chunk]))
        stores[-1].start()
    for store in stores:
        store.wait()


def pack_kernel(points_ref, out_ref):
    rows = 8
    segs = points_ref.shape[1]
    out_ref[...] = jnp.zeros_like(out_ref)

    def one_block(b, carry):
        here = pl.ds(pl.multiple_of(b * rows, rows), rows)
        x, y, z = points_ref[0, here], points_ref[1, here], points_ref[2, here]
        square = 1.0 + 2.0 * (x * x + y * y + z * z)
        for row, value in enumerate((x, y, z, jnp.ones_like(x), square)):
            for half in range(x.shape[1] // 128):
                lanes = slice(half * 128, half * 128 + 128)
                out_ref[half, pl.ds(b * rows * rows + row, rows, stride=rows), :] = value[:, lanes]
        return carry

    lax.fori_loop(0, segs // rows, one_block, 0, unroll=2)


def pieces(value):
    first = value.astype(jnp.bfloat16).astype(jnp.float32)
    rest = value - first
    second = rest.astype(jnp.bfloat16).astype(jnp.float32)
    return (first, second, rest - second)


def node_side(fetched_ref, start, step):
    raw = fetched_ref[pl.ds(start, 6, stride=step), :]
    raw = jnp.concatenate([raw, jnp.zeros((2, raw.shape[1]), jnp.float32)], axis=0)
    row = lax.broadcasted_iota(jnp.int32, raw.shape, 0)
    coord = jnp.where(row < 3, raw, 0.0)
    square = 2.0 * jnp.sum(coord * coord, axis=0, keepdims=True)
    extended = jnp.where(row == 3, square, jnp.where(row == 4, 1.0, -4.0 * coord))
    a, b, c = pieces(extended)
    stacked = jnp.concatenate([a, a, b, b, a, c], axis=0)
    disp = jnp.where(row == 0, 1.0, jnp.where(row < 5, 0.0, pltpu.roll(raw, 2, 0)))
    high = disp.astype(jnp.bfloat16).astype(jnp.float32)
    lhs = jnp.concatenate([high, disp - high], axis=0)
    lhs = jnp.concatenate([lhs, lhs], axis=1).astype(jnp.bfloat16)
    return stacked.astype(jnp.bfloat16).T, lhs


def points_of(points_ref, s):
    here = pl.ds(pl.multiple_of(s * 8, 8), 8)
    return jnp.concatenate([points_ref[h, here] for h in range(points_ref.shape[0])], axis=1)


def point_side(points):
    a, b, c = pieces(points)
    return jnp.concatenate([a, b, a, b, c, a], axis=0).astype(jnp.bfloat16)


def kernel_values(node_op, point_op):
    dist = jnp.dot(node_op, point_op, preferred_element_type=jnp.float32)
    value = 1.0 / dist
    high = value.astype(jnp.bfloat16)
    low = (value - high.astype(jnp.float32)).astype(jnp.bfloat16)
    return jnp.concatenate([high, low], axis=0)


def stage_a(s, start, step, fetched_ref, points_ref, both_ref, lhs_ref, i):
    node_op, lhs = node_side(fetched_ref, start, step)
    lhs_ref[i] = lhs
    both_ref[i] = kernel_values(node_op, point_side(points_of(points_ref, s)))


def sums_of(both_ref, lhs_ref, i):
    sums = jnp.dot(lhs_ref[i], both_ref[i], preferred_element_type=jnp.float32)
    return sums[:8] + sums[8:]


def primary_pass(capacity, follow, refs):
    plan_ref, fetched_ref, points_ref, filled_ref, both_ref, lhs_ref = refs
    segs = plan_ref.shape[1]

    def first(s, i):
        stage_a(s, plan_ref[0, s], capacity, fetched_ref, points_ref, both_ref, lhs_ref, i)

    def second(s, i):
        sums = sums_of(both_ref, lhs_ref, i)
        value = sums * (1.0 / sums[0:1])
        for h in range(filled_ref.shape[0]):
            filled_ref[h, pl.ds(s * 8 + 5, 3), :] = value[5:8, h * 128 : (h + 1) * 128]

    for i in range(WIDE):
        first(i, i)

    def one_group(g, last):
        base = g * (2 * WIDE)
        for i in range(WIDE):
            second(base + i, i)
            first(base + WIDE + i, WIDE + i)
        for i in range(WIDE):
            second(base + WIDE + i, WIDE + i)
            if last:
                follow(i)
            else:
                first(base + 2 * WIDE + i, i)

    groups = segs // (2 * WIDE)

    def full_group(g, carry):
        one_group(g, False)
        return carry

    lax.fori_loop(0, groups - 1, full_group, 0)
    one_group(groups - 1, True)


def secondary_pass(step, apart, base_row, low, end, sets, refs):
    plan_ref, count_ref, fetched_ref, points_ref, weights_ref, filled_ref = refs[:6]
    out_ref, both_ref, lhs_ref, left_ref = refs[6:]

    def entry(row, place):
        return plan_ref[row, jnp.minimum(low + place, end - 1)]

    def first(place, i):
        s, start = entry(1, place), entry(2, place)
        stage_a(s, start, step, fetched_ref, points_ref, both_ref, lhs_ref, i)

    def second(place, i):
        s = entry(1, place)
        sums = sums_of(both_ref, lhs_ref, i)
        inverse = 1.0 / sums[0:1]
        weights = weights_ref[pl.ds(s, 1), :]
        position = lax.broadcasted_iota(jnp.int32, weights.shape, 1)
        weights = jnp.where(position < count_ref[s], weights, 0.0)
        gap = (weights * inverse) * (sums * inverse - points_of(filled_ref, s))
        high = gap.astype(jnp.bfloat16).astype(jnp.float32)
        left_ref[i] = jnp.concatenate([high, gap - high], axis=0).astype(jnp.bfloat16)

    def third(place, i):
        left, both = left_ref[i], both_ref[i]
        half = both.shape[0] // 2
        if i % 2 == 0:
            result = dot_last(left, both)
            result = result[:8] + result[8:]
            result = result[:, :half] + result[:, half:]
        else:
            result = dot_last(both, left)
            result = (result[:half] + result[half:]).T
            result = result[:8] + result[8:]
        out_ref[pl.ds(entry(base_row, place), 3, stride=apart), :] = result[5:8]

    def begin(i):
        if i < 2 * sets:
            first(i, i)

    def one_group(g, last):
        base = g * (3 * sets)
        for phase in range(3):
            for i in range(sets):
                a, b, c = (phase * sets + sets * t + i for t in (2, 1, 0))
                third(base + c, c)
                if not last or b < 3 * sets:
                    second(base + b, b % (3 * sets))
                if not last or a < 3 * sets:
                    first(base + a, a % (3 * sets))

    def finish():
        for i in range(sets):
            second(i, i)
        groups = (end - low + 3 * sets - 1) // (3 * sets)

        def full_group(g, carry):
            one_group(g, False)
            return carry

        lax.fori_loop(0, groups - 1, full_group, 0)
        one_group(groups - 1, True)

    return begin, finish


def early_kernel(capacity, plan_ref, count_ref, fetched_ref, points_ref, weights_ref, *refs):
    filled_ref, out_ref, both_ref, lhs_ref, left_ref = refs
    out_ref[...] = jnp.zeros_like(out_ref)
    filled_ref[...] = points_ref[...]
    begin, finish = secondary_pass(
        1,
        1,
        5,
        0,
        plan_ref[4, 0],
        EARLY_SETS,
        (plan_ref, count_ref, fetched_ref, points_ref, weights_ref, filled_ref)
        + (out_ref, both_ref, lhs_ref, left_ref),
    )
    primary_pass(
        capacity, begin, (plan_ref, fetched_ref, points_ref, filled_ref, both_ref, lhs_ref)
    )
    finish()


def late_kernel(capacity, plan_ref, count_ref, fetched_ref, points_ref, *refs):
    far_weights_ref, before_ref, out_ref, both_ref, lhs_ref, left_ref, weights_ref, sem = refs
    load = pltpu.make_async_copy(far_weights_ref, weights_ref, sem)
    load.start()
    out_ref[...] = jnp.zeros_like(out_ref)
    for row in range(0, before_ref.shape[0], 8):
        out_ref[pl.ds(row * capacity, 8, stride=capacity), :] = before_ref[row : row + 8, :]
    begin, finish = secondary_pass(
        capacity - 1,
        capacity,
        3,
        plan_ref[4, 0],
        plan_ref.shape[1],
        LATE_SETS,
        (plan_ref, count_ref, fetched_ref, points_ref, weights_ref, points_ref)
        + (out_ref, both_ref, lhs_ref, left_ref),
    )
    for i in range(2 * LATE_SETS):
        begin(i)
    load.wait()
    finish()


def assemble_kernel(capacity, blocks, ids_ref, in_ref, out_ref, near_ref, sems):
    devices = ids_ref.shape[1]
    block = 8 * lax.broadcasted_iota(jnp.int32, (blocks, devices), 0)
    nodes = in_ref.shape[1]
    select = [
        jnp.where(block == ids_ref[rank : rank + 1, :], 1.0, 0.0) for rank in range(capacity)
    ]
    select = jnp.concatenate(select, axis=1).astype(jnp.bfloat16)
    step = 3 * capacity
    stores = []
    for components in ((0, 1), (2,)):
        rows = []
        for rank in range(capacity):
            parts = [
                in_ref[pl.ds(c * capacity + rank, devices, stride=step), :] for c in components
            ]
            rows.append(jnp.concatenate(parts, axis=1))
        total = None
        for piece in pieces(jnp.concatenate(rows, axis=0)):
            term = jnp.dot(select, piece.astype(jnp.bfloat16), preferred_element_type=jnp.float32)
            total = term if total is None else total + term
        for i, c in enumerate(components):
            near_ref[c * blocks : (c + 1) * blocks, :] = total[:, i * nodes : (i + 1) * nodes]
        here = pl.ds(components[0] * blocks, len(components) * blocks)
        stores.append(
            pltpu.make_async_copy(near_ref.at[here], out_ref.at[here], sems.at[len(stores)])
        )
        stores[-1].start()
    for store in stores:
        store.wait()


def body(node_coords, node_disp, qpoints, qweights, qcount, sec_block, pri_block):
    devices = lax.axis_size("gx") * lax.axis_size("gy")
    blocks = node_coords.shape[0]
    nodes = node_coords.shape[2]
    segs = qpoints.shape[0]
    quad = qpoints.shape[2]
    slots = 2 * segs
    cap = slots // devices
    f32 = jnp.float32
    smem = pl.BlockSpec(memory_space=pltpu.SMEM)
    vmem = pl.BlockSpec(memory_space=pltpu.VMEM)

    limit = pltpu.CompilerParams(vmem_limit_bytes=16 * 1024 * 1024)

    def near(value):
        return pltpu.with_memory_space_constraint(value, pltpu.VMEM)

    def far(value):
        return pltpu.with_memory_space_constraint(value, pltpu.HBM)

    def exchange(value):
        return lax.all_to_all(value, AXES, split_axis=0, concat_axis=0, tiled=True)

    request, route = pl.pallas_call(
        functools.partial(route_kernel, devices, cap, blocks),
        out_shape=(jax.ShapeDtypeStruct((devices, 128), f32), jax.ShapeDtypeStruct((4, segs), f32)),
        in_specs=[vmem, vmem],
        out_specs=(vmem, vmem),
        compiler_params=limit,
    )(far(sec_block.reshape(1, segs)), far(pri_block.reshape(1, segs)))
    plan = pl.pallas_call(
        functools.partial(order_kernel, cap),
        out_shape=jax.ShapeDtypeStruct((8, segs), jnp.int32),
        in_specs=[vmem],
        out_specs=vmem,
        compiler_params=limit,
    )(route)
    xc = jnp.transpose(node_coords, (1, 0, 2)).reshape(3 * blocks, nodes)
    xu = jnp.transpose(node_disp, (1, 0, 2)).reshape(3 * blocks, nodes)
    hbm = pl.BlockSpec(memory_space=pltpu.HBM)
    table = pl.pallas_call(
        table_kernel,
        out_shape=pltpu.VMEM((8 * blocks, nodes), f32),
        in_specs=[vmem, vmem],
        out_specs=vmem,
        compiler_params=limit,
    )(far(xc), far(xu))
    received = exchange(request.reshape(devices, 1, 128)).reshape(devices, 128)

    def gather(first, rows):
        out, turned = pl.pallas_call(
            functools.partial(gather_kernel, devices, cap, first),
            out_shape=(
                pltpu.HBM((devices * rows, nodes), f32),
                jax.ShapeDtypeStruct((2 * cap, devices), jnp.int32),
            ),
            in_specs=[vmem, vmem],
            out_specs=(hbm, vmem),
            scratch_shapes=[
                pltpu.VMEM((devices * rows, nodes), f32),
                pltpu.SMEM((2 * cap, devices), jnp.int32),
                pltpu.SemaphoreType.DMA,
                pltpu.SemaphoreType.DMA((CHUNKS,)),
            ],
            compiler_params=limit,
        )(received, near(table))
        return out.reshape(devices, rows // 2, 2, nodes), turned

    out1, turned = gather(True, 6 * cap + 6)
    out2, _ = gather(False, 6 * cap - 6)
    in1 = near(exchange(out1).reshape(-1, nodes))
    in2 = near(exchange(out2).reshape(-1, nodes))
    points = pl.pallas_call(
        pack_kernel,
        out_shape=pltpu.VMEM((quad // 128, segs * 8, 128), f32),
        in_specs=[vmem],
        out_specs=vmem,
        compiler_params=limit,
    )(jnp.transpose(qpoints, (1, 0, 2)))
    points = near(points)

    def scratch(count):
        return [
            pltpu.VMEM((count, 2 * nodes, quad), jnp.bfloat16),
            pltpu.VMEM((count, 16, 2 * nodes), jnp.bfloat16),
            pltpu.VMEM((count, 16, quad), jnp.bfloat16),
        ]

    filled, parcels = pl.pallas_call(
        functools.partial(early_kernel, cap),
        out_shape=(
            pltpu.VMEM((quad // 128, segs * 8, 128), f32),
            pltpu.HBM((devices * 3, nodes), f32),
        ),
        in_specs=[smem, smem, vmem, vmem, vmem],
        out_specs=(vmem, vmem),
        scratch_shapes=scratch(max(2 * WIDE, 3 * EARLY_SETS)),
        input_output_aliases={3: 0},
        compiler_params=limit,
    )(plan, qcount, in1, points, far(qweights))
    parcels = pl.pallas_call(
        functools.partial(late_kernel, cap),
        out_shape=pltpu.VMEM((devices * 3 * cap, nodes), f32),
        in_specs=[smem, smem, vmem, vmem, hbm, vmem],
        out_specs=vmem,
        scratch_shapes=scratch(3 * LATE_SETS)
        + [pltpu.VMEM((segs, quad), f32), pltpu.SemaphoreType.DMA],
        compiler_params=limit,
    )(plan, qcount, in2, near(filled), far(qweights), far(parcels))
    incoming = exchange(parcels.reshape(devices, 3, cap, nodes)).reshape(-1, nodes)
    gap = pl.pallas_call(
        functools.partial(assemble_kernel, cap, blocks),
        out_shape=jax.ShapeDtypeStruct((3 * blocks, nodes), f32),
        in_specs=[vmem, vmem],
        out_specs=hbm,
        scratch_shapes=[
            pltpu.VMEM((3 * blocks, nodes), f32),
            pltpu.SemaphoreType.DMA((2,)),
        ],
        compiler_params=limit,
    )(turned, near(incoming))
    return jnp.transpose(gap.reshape(3, blocks, nodes), (1, 0, 2))


def solution(mesh):
    split3 = P(AXES, None, None)
    placed = (split3, split3, split3, P(AXES, None), P(AXES), P(AXES), P(AXES))
    return jax.shard_map(body, mesh=mesh, in_specs=placed, out_specs=split3, check_vma=False)
```

```python
import functools
import jax
import jax.numpy as jnp
from jax import lax
from jax.experimental import pallas as pl
from jax.experimental.pallas import tpu as pltpu
from jax.sharding import PartitionSpec as P

AXES = ("gx", "gy")
WIDE = 16
EARLY_SETS = 7
LATE_SETS = 8
CHUNKS = 4


def strict_upper(size):
    row = lax.broadcasted_iota(jnp.int32, (size, size), 0)
    column = lax.broadcasted_iota(jnp.int32, (size, size), 1)
    return jnp.where(row < column, 1.0, 0.0).astype(jnp.bfloat16)


def dot_last(left, right):
    return lax.dot_general(
        left, right, (((1,), (1,)), ((), ())), preferred_element_type=jnp.float32
    )


def plan_kernel(devices, capacity, blocks, sec_ref, pri_ref, plan_ref, request_ref):
    segs = sec_ref.shape[1]
    upper = strict_upper(segs)
    device = lax.broadcasted_iota(jnp.int32, (devices, segs), 0).astype(jnp.float32)
    column = lax.broadcasted_iota(jnp.int32, (request_ref.shape[1], segs), 0).astype(jnp.float32)
    request = jnp.zeros(request_ref.shape, jnp.float32)
    routes = []
    for side, ref in enumerate((sec_ref, pri_ref)):
        ids = ref[...].astype(jnp.float32)
        owner = jnp.floor((ids + 0.5) * (1.0 / blocks))
        local = ids - owner * blocks
        mine = jnp.where(device == owner, 1.0, 0.0)
        narrow = mine.astype(jnp.bfloat16)
        before = jnp.dot(narrow, upper, preferred_element_type=jnp.float32)
        rank = jnp.sum(mine * before, axis=0, keepdims=True)
        coarse = jnp.floor(local * (1.0 / 16.0)) * 16.0
        here = column == rank + side * capacity
        for part in (coarse, local - coarse):
            request += dot_last(narrow, jnp.where(here, 8.0 * part, 0.0).astype(jnp.bfloat16))
        routes.append((owner, rank))
    request_ref[...] = request

    (sec_owner, sec_rank), (pri_owner, pri_rank) = routes
    early = jnp.where(sec_rank == 0.0, 1.0, 0.0)
    spread = jnp.broadcast_to(early, (16, segs)).astype(jnp.bfloat16)
    ahead = jnp.dot(spread, upper, preferred_element_type=jnp.float32)[:1]
    count = jnp.sum(early, axis=1, keepdims=True)
    number = lax.broadcasted_iota(jnp.int32, (1, segs), 1).astype(jnp.float32)
    place = jnp.where(sec_rank == 0.0, ahead, count + number - ahead)
    target = lax.broadcasted_iota(jnp.int32, (segs, segs), 0).astype(jnp.float32)
    moved = jnp.where(target == place, 1.0, 0.0).astype(jnp.bfloat16)
    row = lax.broadcasted_iota(jnp.int32, (16, segs), 0)
    values = jnp.where(row == 0, number, jnp.where(row == 1, sec_owner, sec_rank))
    values = dot_last(values.astype(jnp.bfloat16), moved)
    seg, dev, rank = values[0:1], values[1:2], values[2:3]
    start = jnp.where(
        rank == 0.0,
        dev * (6 * capacity + 6) + 6 * capacity,
        dev * (6 * capacity - 6) + (rank - 1.0),
    )
    rows = (
        pri_owner * (6 * capacity + 6) + pri_rank,
        seg,
        start,
        dev * (3 * capacity) + rank,
        jnp.broadcast_to(count, (1, segs)),
        dev * 3.0,
    )
    plan_ref[...] = jnp.zeros_like(plan_ref)
    for i, value in enumerate(rows):
        plan_ref[i : i + 1, :] = value.astype(jnp.int32)


def table_kernel(xc_ref, xu_ref, out_ref):
    blocks = xc_ref.shape[0] // 3

    def one_block(b, carry):
        for half, ref in enumerate((xc_ref, xu_ref)):
            for c in range(3):
                here = pl.ds(pl.multiple_of(c * blocks + b * 8, 8), 8)
                out_ref[pl.ds(b * 64 + 3 * half + c, 8, stride=8), :] = ref[here, :]
        return carry

    lax.fori_loop(0, blocks // 8, one_block, 0, unroll=4)


def gather_kernel(devices, capacity, first, ids_ref, table_ref, *refs):
    far_ref, turned_ref, near_ref, local_ref, sem, sems = refs
    turned_ref[...] = ids_ref[...].T[: 2 * capacity].astype(jnp.int32)
    copy = pltpu.make_async_copy(turned_ref, local_ref, sem)
    copy.start()
    copy.wait()
    if first:
        parts = [(1, rank, rank, capacity) for rank in range(capacity)]
        parts.append((0, 0, 6 * capacity, 1))
    else:
        parts = [(0, rank, rank - 1, capacity - 1) for rank in range(1, capacity)]
    rows = 6 * len(parts)

    def one_device(dev, carry):
        for side, rank, start, step in parts:
            row = pl.multiple_of(local_ref[side * capacity + rank, dev], 8)
            patch = table_ref[pl.ds(row, 8), :]
            near_ref[pl.ds(dev * rows + start, 6, stride=step), :] = patch[:6]
        return carry

    part = devices // CHUNKS
    stores = []
    for chunk in range(CHUNKS):
        lax.fori_loop(chunk * part, (chunk + 1) * part, one_device, 0, unroll=8)
        here = pl.ds(chunk * part * rows, part * rows)
        stores.append(pltpu.make_async_copy(near_ref.at[here], far_ref.at[here], sems.at[chunk]))
        stores[-1].start()
    for store in stores:
        store.wait()


def pack_kernel(points_ref, out_ref):
    rows = 8
    segs = points_ref.shape[1]
    out_ref[...] = jnp.zeros_like(out_ref)

    def one_block(b, carry):
        here = pl.ds(pl.multiple_of(b * rows, rows), rows)
        x, y, z = points_ref[0, here], points_ref[1, here], points_ref[2, here]
        square = 1.0 + 2.0 * (x * x + y * y + z * z)
        for row, value in enumerate((x, y, z, jnp.ones_like(x), square)):
            for half in range(x.shape[1] // 128):
                lanes = slice(half * 128, half * 128 + 128)
                out_ref[half, pl.ds(b * rows * rows + row, rows, stride=rows), :] = value[:, lanes]
        return carry

    lax.fori_loop(0, segs // rows, one_block, 0, unroll=2)


def pieces(value):
    first = value.astype(jnp.bfloat16).astype(jnp.float32)
    rest = value - first
    second = rest.astype(jnp.bfloat16).astype(jnp.float32)
    return (first, second, rest - second)


def node_side(fetched_ref, start, step):
    raw = fetched_ref[pl.ds(start, 6, stride=step), :]
    raw = jnp.concatenate([raw, jnp.zeros((2, raw.shape[1]), jnp.float32)], axis=0)
    row = lax.broadcasted_iota(jnp.int32, raw.shape, 0)
    coord = jnp.where(row < 3, raw, 0.0)
    square = 2.0 * jnp.sum(coord * coord, axis=0, keepdims=True)
    extended = jnp.where(row == 3, square, jnp.where(row == 4, 1.0, -4.0 * coord))
    a, b, c = pieces(extended)
    stacked = jnp.concatenate([a, a, b, b, a, c], axis=0)
    disp = jnp.where(row < 3, 0.0, jnp.where(row == 6, 1.0, raw))
    high = disp.astype(jnp.bfloat16).astype(jnp.float32)
    lhs = jnp.concatenate([high, disp - high], axis=0)
    lhs = jnp.concatenate([lhs, lhs], axis=1).astype(jnp.bfloat16)
    return stacked.astype(jnp.bfloat16).T, lhs


def points_of(points_ref, s):
    here = pl.ds(pl.multiple_of(s * 8, 8), 8)
    return jnp.concatenate([points_ref[h, here] for h in range(points_ref.shape[0])], axis=1)


def point_side(points):
    a, b, c = pieces(points)
    return jnp.concatenate([a, b, a, b, c, a], axis=0).astype(jnp.bfloat16)


def kernel_values(node_op, point_op):
    dist = jnp.dot(node_op, point_op, preferred_element_type=jnp.float32)
    value = 1.0 / dist
    high = value.astype(jnp.bfloat16)
    low = (value - high.astype(jnp.float32)).astype(jnp.bfloat16)
    return jnp.concatenate([high, low], axis=0)


def stage_a(s, start, step, fetched_ref, points_ref, both_ref, lhs_ref, i):
    node_op, lhs = node_side(fetched_ref, start, step)
    lhs_ref[i] = lhs
    both_ref[i] = kernel_values(node_op, point_side(points_of(points_ref, s)))


def sums_of(both_ref, lhs_ref, i):
    sums = jnp.dot(lhs_ref[i], both_ref[i], preferred_element_type=jnp.float32)
    return sums[:8] + sums[8:]


def primary_pass(capacity, follow, refs):
    plan_ref, fetched_ref, points_ref, other_ref, both_ref, lhs_ref = refs
    segs = plan_ref.shape[1]

    def first(s, i):
        stage_a(s, plan_ref[0, s], capacity, fetched_ref, points_ref, both_ref, lhs_ref, i)

    def second(s, i):
        sums = sums_of(both_ref, lhs_ref, i)
        other_ref[s] = sums * (1.0 / sums[6:7])

    for i in range(WIDE):
        first(i, i)

    def one_group(g, last):
        base = g * (2 * WIDE)
        for i in range(WIDE):
            second(base + i, i)
            first(base + WIDE + i, WIDE + i)
        for i in range(WIDE):
            second(base + WIDE + i, WIDE + i)
            if last:
                follow(i)
            else:
                first(base + 2 * WIDE + i, i)

    groups = segs // (2 * WIDE)

    def full_group(g, carry):
        one_group(g, False)
        return carry

    lax.fori_loop(0, groups - 1, full_group, 0)
    one_group(groups - 1, True)


def secondary_pass(step, apart, base_row, low, end, sets, refs):
    plan_ref, count_ref, fetched_ref, points_ref, weights_ref, other_ref = refs[:6]
    out_ref, both_ref, lhs_ref, left_ref = refs[6:]

    def entry(row, place):
        return plan_ref[row, jnp.minimum(low + place, end - 1)]

    def first(place, i):
        s, start = entry(1, place), entry(2, place)
        stage_a(s, start, step, fetched_ref, points_ref, both_ref, lhs_ref, i)

    def second(place, i):
        s = entry(1, place)
        sums = sums_of(both_ref, lhs_ref, i)
        inverse = 1.0 / sums[6:7]
        weights = weights_ref[pl.ds(s, 1), :]
        position = lax.broadcasted_iota(jnp.int32, weights.shape, 1)
        weights = jnp.where(position < count_ref[s], weights, 0.0)
        gap = (weights * inverse) * (sums * inverse - other_ref[s])
        high = gap.astype(jnp.bfloat16).astype(jnp.float32)
        left_ref[i] = jnp.concatenate([high, gap - high], axis=0).astype(jnp.bfloat16)

    def third(place, i):
        left, both = left_ref[i], both_ref[i]
        half = both.shape[0] // 2
        if i % 2 == 0:
            result = dot_last(left, both)
            result = result[:8] + result[8:]
            result = result[:, :half] + result[:, half:]
        else:
            result = dot_last(both, left)
            result = (result[:half] + result[half:]).T
            result = result[:8] + result[8:]
        out_ref[pl.ds(entry(base_row, place), 3, stride=apart), :] = result[3:6]

    def begin(i):
        if i < 2 * sets:
            first(i, i)

    def one_group(g, last):
        base = g * (3 * sets)
        for phase in range(3):
            for i in range(sets):
                a, b, c = (phase * sets + sets * t + i for t in (2, 1, 0))
                third(base + c, c)
                if not last or b < 3 * sets:
                    second(base + b, b % (3 * sets))
                if not last or a < 3 * sets:
                    first(base + a, a % (3 * sets))

    def finish():
        for i in range(sets):
            second(i, i)
        groups = (end - low + 3 * sets - 1) // (3 * sets)

        def full_group(g, carry):
            one_group(g, False)
            return carry

        lax.fori_loop(0, groups - 1, full_group, 0)
        one_group(groups - 1, True)

    return begin, finish


def early_kernel(capacity, plan_ref, count_ref, fetched_ref, points_ref, far_weights_ref, *refs):
    far_other_ref, out_ref, both_ref, lhs_ref, left_ref, other_ref, weights_ref, sems = refs
    load = pltpu.make_async_copy(far_weights_ref, weights_ref, sems.at[0])
    store = pltpu.make_async_copy(other_ref, far_other_ref, sems.at[1])
    load.start()
    out_ref[...] = jnp.zeros_like(out_ref)
    begin, finish = secondary_pass(
        1,
        1,
        5,
        0,
        plan_ref[4, 0],
        EARLY_SETS,
        (plan_ref, count_ref, fetched_ref, points_ref, weights_ref, other_ref)
        + (out_ref, both_ref, lhs_ref, left_ref),
    )
    primary_pass(
        capacity, begin, (plan_ref, fetched_ref, points_ref, other_ref, both_ref, lhs_ref)
    )
    store.start()
    load.wait()
    finish()
    store.wait()


def late_kernel(capacity, plan_ref, count_ref, fetched_ref, points_ref, *refs):
    far_weights_ref, far_other_ref, before_ref, out_ref = refs[:4]
    both_ref, lhs_ref, left_ref, other_ref, weights_ref, sems = refs[4:]
    loads = [
        pltpu.make_async_copy(far_weights_ref, weights_ref, sems.at[CHUNKS]),
    ]
    part = other_ref.shape[0] // CHUNKS
    for chunk in range(CHUNKS):
        here = pl.ds(chunk * part, part)
        loads.append(
            pltpu.make_async_copy(far_other_ref.at[here], other_ref.at[here], sems.at[chunk])
        )
    for load in loads:
        load.start()
    out_ref[...] = jnp.zeros_like(out_ref)
    for row in range(0, before_ref.shape[0], 8):
        out_ref[pl.ds(row * capacity, 8, stride=capacity), :] = before_ref[row : row + 8, :]

    begin, finish = secondary_pass(
        capacity - 1,
        capacity,
        3,
        plan_ref[4, 0],
        plan_ref.shape[1],
        LATE_SETS,
        (plan_ref, count_ref, fetched_ref, points_ref, weights_ref, other_ref)
        + (out_ref, both_ref, lhs_ref, left_ref),
    )
    for i in range(2 * LATE_SETS):
        begin(i)
    for load in loads:
        load.wait()
    finish()


def assemble_kernel(capacity, blocks, ids_ref, in_ref, out_ref, near_ref, sems):
    devices = ids_ref.shape[1]
    block = 8 * lax.broadcasted_iota(jnp.int32, (blocks, devices), 0)
    nodes = in_ref.shape[1]
    select = [
        jnp.where(block == ids_ref[rank : rank + 1, :], 1.0, 0.0) for rank in range(capacity)
    ]
    select = jnp.concatenate(select, axis=1).astype(jnp.bfloat16)
    step = 3 * capacity
    stores = []
    for components in ((0, 1), (2,)):
        rows = []
        for rank in range(capacity):
            parts = [
                in_ref[pl.ds(c * capacity + rank, devices, stride=step), :] for c in components
            ]
            rows.append(jnp.concatenate(parts, axis=1))
        total = None
        for piece in pieces(jnp.concatenate(rows, axis=0)):
            term = jnp.dot(select, piece.astype(jnp.bfloat16), preferred_element_type=jnp.float32)
            total = term if total is None else total + term
        for i, c in enumerate(components):
            near_ref[c * blocks : (c + 1) * blocks, :] = total[:, i * nodes : (i + 1) * nodes]
        here = pl.ds(components[0] * blocks, len(components) * blocks)
        stores.append(
            pltpu.make_async_copy(near_ref.at[here], out_ref.at[here], sems.at[len(stores)])
        )
        stores[-1].start()
    for store in stores:
        store.wait()


def body(node_coords, node_disp, qpoints, qweights, qcount, sec_block, pri_block):
    devices = lax.axis_size("gx") * lax.axis_size("gy")
    blocks = node_coords.shape[0]
    nodes = node_coords.shape[2]
    segs = qpoints.shape[0]
    quad = qpoints.shape[2]
    slots = 2 * segs
    cap = slots // devices
    f32 = jnp.float32
    smem = pl.BlockSpec(memory_space=pltpu.SMEM)
    vmem = pl.BlockSpec(memory_space=pltpu.VMEM)

    limit = pltpu.CompilerParams(vmem_limit_bytes=16 * 1024 * 1024)

    def near(value):
        return pltpu.with_memory_space_constraint(value, pltpu.VMEM)

    def far(value):
        return pltpu.with_memory_space_constraint(value, pltpu.HBM)

    def exchange(value):
        return lax.all_to_all(value, AXES, split_axis=0, concat_axis=0, tiled=True)

    plan, request = pl.pallas_call(
        functools.partial(plan_kernel, devices, cap, blocks),
        out_shape=(
            jax.ShapeDtypeStruct((8, segs), jnp.int32),
            jax.ShapeDtypeStruct((devices, 128), f32),
        ),
        in_specs=[vmem, vmem],
        out_specs=(vmem, vmem),
        compiler_params=limit,
    )(far(sec_block.reshape(1, segs)), far(pri_block.reshape(1, segs)))
    xc = jnp.transpose(node_coords, (1, 0, 2)).reshape(3 * blocks, nodes)
    xu = jnp.transpose(node_disp, (1, 0, 2)).reshape(3 * blocks, nodes)
    hbm = pl.BlockSpec(memory_space=pltpu.HBM)
    table = pl.pallas_call(
        table_kernel,
        out_shape=pltpu.VMEM((8 * blocks, nodes), f32),
        in_specs=[vmem, vmem],
        out_specs=vmem,
        compiler_params=limit,
    )(far(xc), far(xu))
    received = exchange(request.reshape(devices, 1, 128)).reshape(devices, 128)

    def gather(first, rows):
        out, turned = pl.pallas_call(
            functools.partial(gather_kernel, devices, cap, first),
            out_shape=(
                pltpu.HBM((devices * rows, nodes), f32),
                jax.ShapeDtypeStruct((2 * cap, devices), jnp.int32),
            ),
            in_specs=[vmem, vmem],
            out_specs=(hbm, vmem),
            scratch_shapes=[
                pltpu.VMEM((devices * rows, nodes), f32),
                pltpu.SMEM((2 * cap, devices), jnp.int32),
                pltpu.SemaphoreType.DMA,
                pltpu.SemaphoreType.DMA((CHUNKS,)),
            ],
            compiler_params=limit,
        )(received, near(table))
        return out.reshape(devices, rows // 2, 2, nodes), turned

    out1, turned = gather(True, 6 * cap + 6)
    out2, _ = gather(False, 6 * cap - 6)
    in1 = near(exchange(out1).reshape(-1, nodes))
    in2 = near(exchange(out2).reshape(-1, nodes))
    points = pl.pallas_call(
        pack_kernel,
        out_shape=pltpu.VMEM((quad // 128, segs * 8, 128), f32),
        in_specs=[vmem],
        out_specs=vmem,
        compiler_params=limit,
    )(jnp.transpose(qpoints, (1, 0, 2)))
    points = near(points)

    def scratch(count, sems):
        return [
            pltpu.VMEM((count, 2 * nodes, quad), jnp.bfloat16),
            pltpu.VMEM((count, 16, 2 * nodes), jnp.bfloat16),
            pltpu.VMEM((count, 16, quad), jnp.bfloat16),
            pltpu.VMEM((segs, 8, quad), f32),
            pltpu.VMEM((segs, quad), f32),
            pltpu.SemaphoreType.DMA((sems,)),
        ]

    weights = far(qweights)
    other, parcels = pl.pallas_call(
        functools.partial(early_kernel, cap),
        out_shape=(
            pltpu.HBM((segs, 8, quad), f32),
            jax.ShapeDtypeStruct((devices * 3, nodes), f32),
        ),
        in_specs=[smem, smem, vmem, vmem, hbm],
        out_specs=(hbm, vmem),
        scratch_shapes=scratch(max(2 * WIDE, 3 * EARLY_SETS), 2),
        compiler_params=limit,
    )(plan, qcount, in1, points, weights)
    parcels = pl.pallas_call(
        functools.partial(late_kernel, cap),
        out_shape=pltpu.VMEM((devices * 3 * cap, nodes), f32),
        in_specs=[smem, smem, vmem, vmem, hbm, hbm, vmem],
        out_specs=vmem,
        scratch_shapes=scratch(3 * LATE_SETS, CHUNKS + 1),
        compiler_params=limit,
    )(plan, qcount, in2, points, weights, far(other), parcels)
    incoming = exchange(parcels.reshape(devices, 3, cap, nodes)).reshape(-1, nodes)
    gap = pl.pallas_call(
        functools.partial(assemble_kernel, cap, blocks),
        out_shape=jax.ShapeDtypeStruct((3 * blocks, nodes), f32),
        in_specs=[vmem, vmem],
        out_specs=hbm,
        scratch_shapes=[
            pltpu.VMEM((3 * blocks, nodes), f32),
            pltpu.SemaphoreType.DMA((2,)),
        ],
        compiler_params=limit,
    )(turned, near(incoming))
    return jnp.transpose(gap.reshape(3, blocks, nodes), (1, 0, 2))


def solution(mesh):
    split3 = P(AXES, None, None)
    placed = (split3, split3, split3, P(AXES, None), P(AXES), P(AXES), P(AXES))
    return jax.shard_map(body, mesh=mesh, in_specs=placed, out_specs=split3, check_vma=False)
```
